32 devices in a mesh: grp: 2 (over y), gy: 4 (over z), gx: 2 (over x), gz: 2 (over core).
Axes of the slice: x: 2, y: 2, z: 4, core: 2. Of those that a mesh axis runs over, the one named last changes fastest.
Arguments:
- pair: bfloat16 [1024, 512, 128], P(('grp', 'gx', 'gz'), 'gy'), parts along dimension 0, may hold values from -6 to 6
- lengths: int32 [2], P('grp'), parts along dimension 0, may hold values from 256 to 512
- ln_gain: float32 [128], replicated, may hold values from 0.1 to 1.9
- ln_bias: float32 [128], replicated, may hold values from -3 to 3
- w_ab: bfloat16 [128, 512], replicated, may hold values from -0.5 to 0.5
- w_gate: bfloat16 [128, 128], replicated, may hold values from -0.5 to 0.5
- out_gain: float32 [128], replicated, may hold values from 0.1 to 1.9
- out_bias: float32 [128], replicated, may hold values from -3 to 3
- w_out: bfloat16 [128, 128], replicated, may hold values from -0.5 to 0.5
Outputs:
- update: bfloat16 [1024, 512, 128], P(('grp', 'gx', 'gz'), 'gy'), parts along dimension 0
The draws below stay inside these ranges and needn't reach their ends.
There are 2 independent parts, one for each index of `grp`. The reference program is written for one: setup_inputs(seed, part) draws one part's arguments, and reference() takes and returns one part's arrays. A program takes and returns all parts, laid end to end along the dimension named above; an argument that names none is the same for every part. Nothing has to cross between parts.
Inputs may be any that keep to these rules, and one draw needn't show every extreme that they name: Residues from lengths[0] on are padding.
All inputs are finite; a program needn't handle non-finite values.
Results may differ from the reference program's by a relative error of at most 0.0052.
Values may be sent and summed in bfloat16 or wider, within the bound.
A program may use at most 128 MiB of HBM per device.

```python
import jax
import jax.numpy as jnp
from jax import lax

N = 512
C = 128
CH = 128


def shard_levels(key, dims, pieces, smallest, top_value):
    factor_of, own = 1.0, jax.random.fold_in(key, 6)
    for dim, parts in pieces:
        steps = jnp.exp(jax.random.uniform(jax.random.fold_in(own, dim), (parts,), jnp.float32, smallest / len(pieces), top_value / len(pieces)))
        factor_of = factor_of * jnp.repeat(steps, dims[dim] // parts).reshape([-1 if axis == dim else 1 for axis in range(len(dims))])
    return factor_of


def gaussian(rng, extent, scale, reach, pieces=(), kind=jnp.bfloat16):
    level = shard_levels(rng, extent, pieces, -0.22, 0.18) if pieces else 1.0
    array = jax.random.normal(rng, extent, jnp.float32) * scale * level
    return jnp.minimum(jnp.maximum(array, -reach), reach).astype(kind)


def setup_inputs(seed: int = 0, part: int = 0) -> dict:
    keys = jax.random.split(jax.random.key(seed), 10)
    part_keys = jax.random.split(jax.random.fold_in(keys[9], part), 10)
    pair = gaussian(part_keys[0], (N, N, C), 1.0, 6.0, ((0, 4), (1, 4)))
    lengths = jax.random.randint(part_keys[1], (1,), N // 2, N + 1).astype(jnp.int32)
    ln_gain = jnp.clip(1.0 + 0.18 * jax.random.normal(keys[2], (C,), jnp.float32), 0.1, 1.9)
    ln_bias = gaussian(keys[3], (C,), 0.5, 3.0, (), jnp.float32)
    w_ab = gaussian(keys[4], (C, 4 * CH), C ** -0.5, 0.5)
    w_gate = gaussian(keys[5], (C, C), C ** -0.5, 0.5)
    out_gain = jnp.clip(1.0 + 0.18 * jax.random.normal(keys[6], (CH,), jnp.float32), 0.1, 1.9)
    out_bias = gaussian(keys[7], (CH,), 0.5, 3.0, (), jnp.float32)
    w_out = gaussian(keys[8], (CH, C), CH ** -0.5, 0.5)
    return dict(pair=pair, lengths=lengths, ln_gain=ln_gain, ln_bias=ln_bias, w_ab=w_ab, w_gate=w_gate, out_gain=out_gain, out_bias=out_bias, w_out=w_out)


def layer_norm(values, gain, bias):
    values = values.astype(jnp.float32)
    mean = lax.optimization_barrier(jnp.mean(values, -1, keepdims=True))
    spread = lax.optimization_barrier(jnp.mean(jnp.square(values - mean), -1, keepdims=True))
    return (values - mean) * lax.rsqrt(spread + 1e-05) * gain.astype(jnp.float32) + bias.astype(jnp.float32)

def reference(pair, lengths, ln_gain, ln_bias, w_ab, w_gate, out_gain, out_bias, w_out):
    hidden = w_out.shape[0]
    width = pair.shape[2]
    normed = layer_norm(pair, ln_gain, ln_bias).astype(jnp.bfloat16)
    flat = normed.reshape(N * N, width)
    proj = jnp.dot(flat, w_ab, preferred_element_type=jnp.float32).reshape(N, N, 4 * hidden)
    live = (jnp.arange(N, dtype=jnp.int32) < lengths[0]).astype(jnp.float32)
    pair_mask = (live[:, None] * live[None, :])[..., None]
    left = (pair_mask * jax.nn.sigmoid(proj[..., :hidden]) * proj[..., hidden:2 * hidden]).astype(jnp.bfloat16)
    right = (pair_mask * jax.nn.sigmoid(proj[..., 2 * hidden:3 * hidden]) * proj[..., 3 * hidden:]).astype(jnp.bfloat16)
    triangle = jnp.einsum('ikc,jkc->ijc', left.astype(jnp.float32), right.astype(jnp.float32), precision=lax.Precision.HIGHEST)
    tri_norm = layer_norm(triangle, out_gain, out_bias).astype(jnp.bfloat16)
    gate = jax.nn.sigmoid(jnp.dot(flat, w_gate, preferred_element_type=jnp.float32))
    projected = jnp.dot(tri_norm.reshape(N * N, hidden), w_out, preferred_element_type=jnp.float32)
    return (gate * projected).astype(jnp.bfloat16).reshape(N, N, width)
```

```python
import functools

import jax
import jax.numpy as jnp
from jax import lax
from jax.experimental import pallas as pl
from jax.experimental.pallas import tpu as pltpu
from jax.sharding import PartitionSpec as P

CHUNKS = 2
ROWS = 16


def layer_norm(values, gain, bias):
    values = values.astype(jnp.float32)
    mean = jnp.mean(values, -1, keepdims=True)
    spread = jnp.mean(jnp.square(values - mean), -1, keepdims=True)
    return (values - mean) * lax.rsqrt(spread + 1e-05) * gain + bias


def channel_norm(values, gain, bias):
    mean = jnp.mean(values, 0, keepdims=True)
    spread = jnp.mean(jnp.square(values - mean), 0, keepdims=True)
    return (values - mean) * lax.rsqrt(spread + 1e-05) * gain[:, None, None] + bias[:, None, None]


def gather_body(pair, lengths, ln_gain, ln_bias, w_ab, w_gate, out_gain, out_bias, w_out):
    tile_rows, tile_cols, width = pair.shape
    hidden = w_out.shape[0]
    row_start = lax.axis_index(("gx", "gz")) * tile_rows
    col_index = lax.axis_index("gy")
    col_start = col_index * tile_cols
    normed = layer_norm(pair, ln_gain, ln_bias).astype(jnp.bfloat16)
    flat = normed.reshape(tile_rows * tile_cols, width)
    proj = jnp.dot(flat, w_ab, preferred_element_type=jnp.float32).reshape(
        tile_rows, tile_cols, 4 * hidden
    )
    row_live = (row_start + jnp.arange(tile_rows, dtype=jnp.int32) < lengths[0]).astype(jnp.float32)
    col_live = (col_start + jnp.arange(tile_cols, dtype=jnp.int32) < lengths[0]).astype(jnp.float32)
    pair_mask = (row_live[:, None] * col_live[None, :])[..., None]
    left = (pair_mask * jax.nn.sigmoid(proj[..., :hidden]) * proj[..., hidden : 2 * hidden]).astype(
        jnp.bfloat16
    )
    right = (
        pair_mask * jax.nn.sigmoid(proj[..., 2 * hidden : 3 * hidden]) * proj[..., 3 * hidden :]
    ).astype(jnp.bfloat16)
    left_major = jnp.transpose(left, (2, 0, 1))
    right_major = jnp.transpose(right, (2, 0, 1))
    column_rows = lax.all_gather(right_major, ("gx", "gz"), axis=1, tiled=True)
    right_mine = lax.all_to_all(column_rows, "gy", split_axis=1, concat_axis=2, tiled=True)
    triangle = jnp.einsum(
        "cik,cjk->cij",
        lax.all_gather(left_major, "gy", axis=2, tiled=True),
        right_mine,
        preferred_element_type=jnp.float32,
    )
    tri_norm = channel_norm(triangle, out_gain, out_bias).astype(jnp.bfloat16)
    gate = jax.nn.sigmoid(jnp.dot(flat, w_gate, preferred_element_type=jnp.float32)).reshape(
        tile_rows, tile_cols, width
    )
    projected = jnp.einsum("cij,cd->ijd", tri_norm, w_out, preferred_element_type=jnp.float32)
    return (gate * projected).astype(jnp.bfloat16)


def project_kernel(lengths, starts, pair, gain, bias, w_t, out):
    rows, cols, width = pair.shape
    hidden = out.shape[1]
    flat = pair[...].reshape(rows * cols, width)
    normed = layer_norm(flat, gain[...], bias[...]).astype(jnp.bfloat16)
    proj = lax.dot_general(
        w_t[...], normed, (((1,), (1,)), ((), ())), preferred_element_type=jnp.float32
    )
    lane = lax.broadcasted_iota(jnp.int32, (1, rows * cols), 1)
    row = starts[0] + pl.program_id(0) * rows + lane // cols
    col = starts[1] + lane % cols
    mask = ((row < lengths[0]) & (col < lengths[0])).astype(jnp.float32)
    for side in range(2):
        base = 2 * side * hidden
        value = (
            mask * jax.nn.sigmoid(proj[base : base + hidden]) * proj[base + hidden : base + 2 * hidden]
        )
        out[side] = value.reshape(hidden, rows, cols).astype(jnp.bfloat16)


def exchange_kernel(
    ny, nx, nz, send, out, held, tri, in_send, in_recv, out_send, out_recv, own_sem
):
    n = ny * nx * nz
    hidden, rows, cols = send.shape[1:]
    each = hidden // n
    part = each // CHUNKS
    gy, gx, gz = lax.axis_index("gy"), lax.axis_index("gx"), lax.axis_index("gz")
    me = (gx * nz + gz) * ny + gy

    def where(index):
        tall, wide = index // ny, index % ny
        return (
            {"gy": wide, "gx": tall // nz, "gz": tall % nz},
            pl.ds(pl.multiple_of(tall * rows, rows), rows),
            pl.ds(pl.multiple_of(wide * cols, cols), cols),
        )

    def deal(chunk, step):
        peer = lax.rem(me + step, n)
        _, my_rows, my_cols = where(me)
        slot = chunk * n + step
        return pltpu.make_async_remote_copy(
            src_ref=send.at[:, pl.ds(peer * each + chunk * part, part)],
            dst_ref=held.at[:, pl.ds(chunk * part, part), my_rows, my_cols],
            send_sem=in_send.at[slot],
            recv_sem=in_recv.at[slot],
            device_id=where(peer)[0],
            device_id_type=pl.DeviceIdType.MESH,
        )

    def hand_back(chunk, step):
        peer = lax.rem(me + step, n)
        device, its_rows, its_cols = where(peer)
        slot = chunk * n + step
        return pltpu.make_async_remote_copy(
            src_ref=tri.at[pl.ds(chunk * part, part), its_rows, its_cols],
            dst_ref=out.at[pl.ds(me * each + chunk * part, part)],
            send_sem=out_send.at[slot],
            recv_sem=out_recv.at[slot],
            device_id=device,
            device_id_type=pl.DeviceIdType.MESH,
        )

    def keep_in(chunk):
        _, my_rows, my_cols = where(me)
        return pltpu.make_async_copy(
            send.at[:, pl.ds(me * each + chunk * part, part)],
            held.at[:, pl.ds(chunk * part, part), my_rows, my_cols],
            own_sem.at[chunk],
        )

    def keep_out(chunk):
        _, my_rows, my_cols = where(me)
        return pltpu.make_async_copy(
            tri.at[pl.ds(chunk * part, part), my_rows, my_cols],
            out.at[pl.ds(me * each + chunk * part, part)],
            own_sem.at[CHUNKS + chunk],
        )

    barrier = pltpu.get_barrier_semaphore()
    for step in range(1, n):
        pl.semaphore_signal(
            barrier,
            inc=1,
            device_id=where(lax.rem(me + step, n))[0],
            device_id_type=pl.DeviceIdType.MESH,
        )
    pl.semaphore_wait(barrier, n - 1)

    for chunk in range(CHUNKS):
        for step in range(1, n):
            deal(chunk, step).start()
        keep_in(chunk).start()
    for chunk in range(CHUNKS):
        for step in range(1, n):
            deal(chunk, step).wait_recv()
        keep_in(chunk).wait()

        @pl.loop(chunk * part, (chunk + 1) * part)
        def _(channel):
            tri[channel] = lax.dot_general(
                held[0, channel],
                held[1, channel],
                (((1,), (1,)), ((), ())),
                preferred_element_type=jnp.float32,
            ).astype(jnp.bfloat16)

        for step in range(1, n):
            hand_back(chunk, step).start()
        keep_out(chunk).start()
    for chunk in range(CHUNKS):
        for step in range(1, n):
            hand_back(chunk, step).wait_recv()
            deal(chunk, step).wait_send()
            hand_back(chunk, step).wait_send()
        keep_out(chunk).wait()


def finish_kernel(pair, tri, gain, bias, w_gate, out_gain, out_bias, w_out, out):
    rows, cols, width = pair.shape
    hidden = tri.shape[0]
    flat = pair[...].reshape(rows * cols, width)
    normed = layer_norm(flat, gain[...], bias[...]).astype(jnp.bfloat16)
    gate = jax.nn.sigmoid(jnp.dot(normed, w_gate[...], preferred_element_type=jnp.float32))
    values = tri[...].astype(jnp.float32)
    mean = jnp.mean(values, 0, keepdims=True)
    centred = values - mean
    spread = jnp.mean(jnp.square(centred), 0, keepdims=True)
    scaled = (centred * lax.rsqrt(spread + 1e-05)).reshape(hidden, rows * cols)
    tri_norm = (scaled * out_gain[...] + out_bias[...]).astype(jnp.bfloat16)
    projected = lax.dot_general(
        tri_norm, w_out[...], (((0,), (0,)), ((), ())), preferred_element_type=jnp.float32
    )
    out[...] = (gate * projected).astype(jnp.bfloat16).reshape(rows, cols, width)


def whole(shape):
    return pl.BlockSpec(shape, lambda step: (0,) * len(shape))


def channel_body(sizes, pair, lengths, ln_gain, ln_bias, w_ab, w_gate, out_gain, out_bias, w_out):
    ny, nx, nz = sizes
    n = ny * nx * nz
    tile_rows, tile_cols, width = pair.shape
    hidden = w_out.shape[0]
    starts = jnp.stack(
        [lax.axis_index(("gx", "gz")) * tile_rows, lax.axis_index("gy") * tile_cols]
    ).astype(jnp.int32)
    gain, bias = ln_gain[None, :], ln_bias[None, :]
    smem = pl.BlockSpec(memory_space=pltpu.SMEM)
    steps = tile_rows // ROWS
    sides = pl.pallas_call(
        project_kernel,
        name="project",
        grid=(steps,),
        out_shape=jax.ShapeDtypeStruct((2, hidden, tile_rows, tile_cols), jnp.bfloat16),
        in_specs=[
            smem,
            smem,
            pl.BlockSpec((ROWS, tile_cols, width), lambda step: (step, 0, 0)),
            whole((1, width)),
            whole((1, width)),
            whole((4 * hidden, width)),
        ],
        out_specs=pl.BlockSpec((2, hidden, ROWS, tile_cols), lambda step: (0, 0, step, 0)),
        compiler_params=pltpu.CompilerParams(vmem_limit_bytes=56 * 2**20),
    )(lengths, starts, pair, gain, bias, w_ab.T)
    dma = pltpu.SemaphoreType.DMA
    any_space = pl.BlockSpec(memory_space=pl.ANY)
    triangle = pl.pallas_call(
        functools.partial(exchange_kernel, ny, nx, nz),
        name="exchange",
        out_shape=jax.ShapeDtypeStruct((hidden, tile_rows, tile_cols), jnp.bfloat16),
        in_specs=[any_space],
        out_specs=any_space,
        scratch_shapes=[
            pltpu.VMEM((2, hidden // n, nx * nz * tile_rows, ny * tile_cols), jnp.bfloat16),
            pltpu.VMEM((hidden // n, nx * nz * tile_rows, ny * tile_cols), jnp.bfloat16),
            dma((CHUNKS * n,)),
            dma((CHUNKS * n,)),
            dma((CHUNKS * n,)),
            dma((CHUNKS * n,)),
            dma((2 * CHUNKS,)),
        ],
        compiler_params=pltpu.CompilerParams(
            collective_id=0, has_side_effects=True, vmem_limit_bytes=48 * 2**20
        ),
    )(sides)
    return pl.pallas_call(
        finish_kernel,
        name="finish",
        grid=(steps,),
        out_shape=jax.ShapeDtypeStruct(pair.shape, jnp.bfloat16),
        in_specs=[
            pl.BlockSpec((ROWS, tile_cols, width), lambda step: (step, 0, 0)),
            pl.BlockSpec((hidden, ROWS, tile_cols), lambda step: (0, step, 0)),
            whole((1, width)),
            whole((1, width)),
            whole((width, width)),
            whole((hidden, 1)),
            whole((hidden, 1)),
            whole((hidden, width)),
        ],
        out_specs=pl.BlockSpec((ROWS, tile_cols, width), lambda step: (step, 0, 0)),
        compiler_params=pltpu.CompilerParams(vmem_limit_bytes=56 * 2**20),
    )(pair, triangle, gain, bias, w_gate, out_gain[:, None], out_bias[:, None], w_out)


def body(sizes, pair, *rest):
    ny, nx, nz = sizes
    n = ny * nx * nz
    hidden = rest[-1].shape[0]
    tile_rows, tile_cols, _ = pair.shape
    fits = (
        hidden % (n * CHUNKS) == 0
        and tile_rows == tile_cols
        and ny == nx * nz
        and tile_cols % 128 == 0
    )
    return channel_body(sizes, pair, *rest) if fits else gather_body(pair, *rest)


def solution(mesh):
    in_specs = (P(("grp", "gx", "gz"), "gy", None), P("grp"), P(), P(), P(), P(), P(), P(), P())
    out_specs = P(("grp", "gx", "gz"), "gy", None)
    sizes = (mesh.shape["gy"], mesh.shape["gx"], mesh.shape["gz"])
    return jax.shard_map(
        functools.partial(body, sizes), mesh=mesh, in_specs=in_specs, out_specs=out_specs, check_vma=False
    )
```

```python
import functools

import jax
import jax.numpy as jnp
from jax import lax
from jax.experimental import pallas as pl
from jax.experimental.pallas import tpu as pltpu
from jax.sharding import PartitionSpec as P

CHUNKS = 16
LAG = 2
ROWS = 16


def layer_norm(values, gain, bias):
    values = values.astype(jnp.float32)
    mean = jnp.mean(values, -1, keepdims=True)
    spread = jnp.mean(jnp.square(values - mean), -1, keepdims=True)
    return (values - mean) * lax.rsqrt(spread + 1e-05) * gain + bias


def channel_norm(values, gain, bias):
    mean = jnp.mean(values, 0, keepdims=True)
    spread = jnp.mean(jnp.square(values - mean), 0, keepdims=True)
    return (values - mean) * lax.rsqrt(spread + 1e-05) * gain[:, None, None] + bias[:, None, None]


def gather_body(pair, lengths, ln_gain, ln_bias, w_ab, w_gate, out_gain, out_bias, w_out):
    tile_rows, tile_cols, width = pair.shape
    hidden = w_out.shape[0]
    row_start = lax.axis_index(("gx", "gz")) * tile_rows
    col_index = lax.axis_index("gy")
    col_start = col_index * tile_cols
    normed = layer_norm(pair, ln_gain, ln_bias).astype(jnp.bfloat16)
    flat = normed.reshape(tile_rows * tile_cols, width)
    proj = jnp.dot(flat, w_ab, preferred_element_type=jnp.float32).reshape(
        tile_rows, tile_cols, 4 * hidden
    )
    row_live = (row_start + jnp.arange(tile_rows, dtype=jnp.int32) < lengths[0]).astype(jnp.float32)
    col_live = (col_start + jnp.arange(tile_cols, dtype=jnp.int32) < lengths[0]).astype(jnp.float32)
    pair_mask = (row_live[:, None] * col_live[None, :])[..., None]
    left = (pair_mask * jax.nn.sigmoid(proj[..., :hidden]) * proj[..., hidden : 2 * hidden]).astype(
        jnp.bfloat16
    )
    right = (
        pair_mask * jax.nn.sigmoid(proj[..., 2 * hidden : 3 * hidden]) * proj[..., 3 * hidden :]
    ).astype(jnp.bfloat16)
    left_major = jnp.transpose(left, (2, 0, 1))
    right_major = jnp.transpose(right, (2, 0, 1))
    column_rows = lax.all_gather(right_major, ("gx", "gz"), axis=1, tiled=True)
    right_mine = lax.all_to_all(column_rows, "gy", split_axis=1, concat_axis=2, tiled=True)
    triangle = jnp.einsum(
        "cik,cjk->cij",
        lax.all_gather(left_major, "gy", axis=2, tiled=True),
        right_mine,
        preferred_element_type=jnp.float32,
    )
    tri_norm = channel_norm(triangle, out_gain, out_bias).astype(jnp.bfloat16)
    gate = jax.nn.sigmoid(jnp.dot(flat, w_gate, preferred_element_type=jnp.float32)).reshape(
        tile_rows, tile_cols, width
    )
    projected = jnp.einsum("cij,cd->ijd", tri_norm, w_out, preferred_element_type=jnp.float32)
    return (gate * projected).astype(jnp.bfloat16)


def project_kernel(lengths, starts, pair, gain, bias, w_t, out):
    rows, cols, width = pair.shape
    hidden = out.shape[1]
    flat = pair[...].reshape(rows * cols, width)
    normed = layer_norm(flat, gain[...], bias[...]).astype(jnp.bfloat16)
    proj = lax.dot_general(
        w_t[...], normed, (((1,), (1,)), ((), ())), preferred_element_type=jnp.float32
    )
    lane = lax.broadcasted_iota(jnp.int32, (1, rows * cols), 1)
    row = starts[0] + pl.program_id(0) * rows + lane // cols
    col = starts[1] + lane % cols
    mask = ((row < lengths[0]) & (col < lengths[0])).astype(jnp.float32)
    for side in range(2):
        base = 2 * side * hidden
        value = (
            mask * jax.nn.sigmoid(proj[base : base + hidden]) * proj[base + hidden : base + 2 * hidden]
        )
        out[side] = value.reshape(hidden, rows, cols).astype(jnp.bfloat16)


def exchange_kernel(
    nx,
    nz,
    send,
    out,
    held,
    given,
    taken,
    tri,
    deal_send,
    deal_recv,
    pass_send,
    pass_recv,
    cross_send,
    cross_recv,
    back_send,
    back_recv,
    own_sem,
):
    nr = nx * nz
    hidden, rows, cols = send.shape[1:]
    each = hidden // nr
    chunks = pass_send.shape[0]
    part = each // chunks
    gy, gx, gz = lax.axis_index("gy"), lax.axis_index("gx"), lax.axis_index("gz")
    me = gx * nz + gz
    half = gy // 2
    inner_plane, outer_plane = 1 + half, 3 * half
    inner = gy == inner_plane

    def place(tall, plane):
        return {"gy": plane, "gx": tall // nz, "gz": tall % nz}

    def remote(src, dst, send_sem, recv_sem, device):
        return pltpu.make_async_remote_copy(
            src_ref=src,
            dst_ref=dst,
            send_sem=send_sem,
            recv_sem=recv_sem,
            device_id=device,
            device_id_type=pl.DeviceIdType.MESH,
        )

    def channels(chunk):
        return pl.ds(chunk * part, part)

    def band(tall):
        return pl.ds(pl.multiple_of(tall * rows, rows), rows)

    def columns(plane):
        return pl.ds(pl.multiple_of((plane - 2 * half) * cols, cols), cols)

    def deal(chunk, step):
        peer = lax.rem(me + step, nr)
        return remote(
            send.at[:, pl.ds(peer * each + chunk * part, part)],
            held.at[:, channels(chunk), band(me), pl.ds(0, cols)],
            deal_send.at[chunk, step],
            deal_recv.at[chunk, step],
            place(peer, gy),
        )

    def keep_in(chunk):
        return pltpu.make_async_copy(
            send.at[:, pl.ds(me * each + chunk * part, part)],
            held.at[:, channels(chunk), band(me), pl.ds(0, cols)],
            own_sem.at[0, chunk],
        )

    def pass_on(chunk):
        return remote(
            held.at[:, channels(chunk), :, pl.ds(0, cols)],
            held.at[:, channels(chunk), :, pl.ds(cols, cols)],
            pass_send.at[chunk],
            pass_recv.at[chunk],
            place(me, inner_plane),
        )

    def cross(chunk):
        return remote(
            given.at[channels(chunk)],
            taken.at[channels(chunk)],
            cross_send.at[chunk],
            cross_recv.at[chunk],
            place(me, 3 - gy),
        )

    def hand_back(chunk, step, plane, side):
        peer = lax.rem(me + step, nr)
        return remote(
            tri.at[channels(chunk), band(peer), columns(plane)],
            out.at[pl.ds(me * each + chunk * part, part)],
            back_send.at[side, chunk, step],
            back_recv.at[chunk, step],
            place(peer, plane),
        )

    def keep_out(chunk):
        return pltpu.make_async_copy(
            tri.at[channels(chunk), band(me), columns(inner_plane)],
            out.at[pl.ds(me * each + chunk * part, part)],
            own_sem.at[1, chunk],
        )

    barrier = pltpu.get_barrier_semaphore()
    total = 4 * nr
    index = gy * nr + me
    for step in range(1, total):
        peer = lax.rem(index + step, total)
        pl.semaphore_signal(
            barrier,
            inc=1,
            device_id=place(peer % nr, peer // nr),
            device_id_type=pl.DeviceIdType.MESH,
        )
    pl.semaphore_wait(barrier, total - 1)

    @pl.loop(0, chunks)
    def _(chunk):
        for step in range(1, nr):
            deal(chunk, step).start()
        keep_in(chunk).start()

    def dealt(chunk):
        for step in range(1, nr):
            deal(chunk, step).wait_recv()
        keep_in(chunk).wait()

    def product(channel, which):
        below = pl.ds(pl.multiple_of(which * 2 * cols, 2 * cols), 2 * cols)
        return lax.dot_general(
            held[0, channel],
            held[1, channel, below, :],
            (((1,), (1,)), ((), ())),
            preferred_element_type=jnp.float32,
        )

    @pl.when(jnp.logical_not(inner))
    def _():
        @pl.loop(0, chunks)
        def _(chunk):
            dealt(chunk)
            pass_on(chunk).start()

        @pl.loop(0, chunks)
        def _(chunk):
            for step in range(nr):
                hand_back(chunk, step, outer_plane, 1).wait_recv()
            for step in range(1, nr):
                deal(chunk, step).wait_send()
            pass_on(chunk).wait_send()

    @pl.when(inner)
    def _():
        @pl.loop(0, chunks + LAG)
        def _(turn):
            @pl.when(turn < chunks)
            def _():
                dealt(turn)
                pass_on(turn).wait_recv()

                @pl.loop(turn * part, (turn + 1) * part)
                def _(channel):
                    given[channel] = product(channel, 1 - half).astype(jnp.bfloat16)

                cross(turn).start()

            @pl.when(turn >= LAG)
            def _():
                chunk = turn - LAG
                cross(chunk).wait_recv()

                @pl.loop(chunk * part, (chunk + 1) * part)
                def _(channel):
                    total = product(channel, half) + taken[channel].astype(jnp.float32)
                    tri[channel] = total.astype(jnp.bfloat16)

                for step in range(nr):
                    hand_back(chunk, step, outer_plane, 1).start()
                for step in range(1, nr):
                    hand_back(chunk, step, inner_plane, 0).start()
                keep_out(chunk).start()

        @pl.loop(0, chunks)
        def _(chunk):
            for step in range(1, nr):
                hand_back(chunk, step, inner_plane, 0).wait_recv()
                hand_back(chunk, step, inner_plane, 0).wait_send()
                deal(chunk, step).wait_send()
            for step in range(nr):
                hand_back(chunk, step, outer_plane, 1).wait_send()
            cross(chunk).wait_send()
            keep_out(chunk).wait()


def finish_kernel(pair, tri, gain, bias, w_gate, out_gain, out_bias, w_out, out):
    rows, cols, width = pair.shape
    hidden = tri.shape[0]
    flat = pair[...].reshape(rows * cols, width)
    normed = layer_norm(flat, gain[...], bias[...]).astype(jnp.bfloat16)
    gate = jax.nn.sigmoid(jnp.dot(normed, w_gate[...], preferred_element_type=jnp.float32))
    values = tri[...].astype(jnp.float32)
    mean = jnp.mean(values, 0, keepdims=True)
    centred = values - mean
    spread = jnp.mean(jnp.square(centred), 0, keepdims=True)
    scaled = (centred * lax.rsqrt(spread + 1e-05)).reshape(hidden, rows * cols)
    tri_norm = (scaled * out_gain[...] + out_bias[...]).astype(jnp.bfloat16)
    projected = lax.dot_general(
        tri_norm, w_out[...], (((0,), (0,)), ((), ())), preferred_element_type=jnp.float32
    )
    out[...] = (gate * projected).astype(jnp.bfloat16).reshape(rows, cols, width)


def whole(shape):
    return pl.BlockSpec(shape, lambda step: (0,) * len(shape))


def channel_body(sizes, pair, lengths, ln_gain, ln_bias, w_ab, w_gate, out_gain, out_bias, w_out):
    ny, nx, nz = sizes
    tile_rows, tile_cols, width = pair.shape
    hidden = w_out.shape[0]
    starts = jnp.stack(
        [lax.axis_index(("gx", "gz")) * tile_rows, lax.axis_index("gy") * tile_cols]
    ).astype(jnp.int32)
    gain, bias = ln_gain[None, :], ln_bias[None, :]
    smem = pl.BlockSpec(memory_space=pltpu.SMEM)
    steps = tile_rows // ROWS
    sides = pl.pallas_call(
        project_kernel,
        name="project",
        grid=(steps,),
        out_shape=jax.ShapeDtypeStruct((2, hidden, tile_rows, tile_cols), jnp.bfloat16),
        in_specs=[
            smem,
            smem,
            pl.BlockSpec((ROWS, tile_cols, width), lambda step: (step, 0, 0)),
            whole((1, width)),
            whole((1, width)),
            whole((4 * hidden, width)),
        ],
        out_specs=pl.BlockSpec((2, hidden, ROWS, tile_cols), lambda step: (0, 0, step, 0)),
        compiler_params=pltpu.CompilerParams(vmem_limit_bytes=56 * 2**20),
    )(lengths, starts, pair, gain, bias, w_ab.T)
    dma = pltpu.SemaphoreType.DMA
    any_space = pl.BlockSpec(memory_space=pl.ANY)
    nr = nx * nz
    each, side = hidden // nr, nr * tile_rows
    triangle = pl.pallas_call(
        functools.partial(exchange_kernel, nx, nz),
        name="exchange",
        out_shape=jax.ShapeDtypeStruct((hidden, tile_rows, tile_cols), jnp.bfloat16),
        in_specs=[any_space],
        out_specs=any_space,
        scratch_shapes=[
            pltpu.VMEM((2, each, side, 2 * tile_cols), jnp.bfloat16),
            pltpu.VMEM((each, side, 2 * tile_cols), jnp.bfloat16),
            pltpu.VMEM((each, side, 2 * tile_cols), jnp.bfloat16),
            pltpu.VMEM((each, side, 2 * tile_cols), jnp.bfloat16),
            dma((CHUNKS, nr)),
            dma((CHUNKS, nr)),
            dma((CHUNKS,)),
            dma((CHUNKS,)),
            dma((CHUNKS,)),
            dma((CHUNKS,)),
            dma((2, CHUNKS, nr)),
            dma((CHUNKS, nr)),
            dma((2, CHUNKS)),
        ],
        compiler_params=pltpu.CompilerParams(
            collective_id=0, has_side_effects=True, vmem_limit_bytes=56 * 2**20
        ),
    )(sides)
    return pl.pallas_call(
        finish_kernel,
        name="finish",
        grid=(steps,),
        out_shape=jax.ShapeDtypeStruct(pair.shape, jnp.bfloat16),
        in_specs=[
            pl.BlockSpec((ROWS, tile_cols, width), lambda step: (step, 0, 0)),
            pl.BlockSpec((hidden, ROWS, tile_cols), lambda step: (0, step, 0)),
            whole((1, width)),
            whole((1, width)),
            whole((width, width)),
            whole((hidden, 1)),
            whole((hidden, 1)),
            whole((hidden, width)),
        ],
        out_specs=pl.BlockSpec((ROWS, tile_cols, width), lambda step: (step, 0, 0)),
        compiler_params=pltpu.CompilerParams(vmem_limit_bytes=56 * 2**20),
    )(pair, triangle, gain, bias, w_gate, out_gain[:, None], out_bias[:, None], w_out)


def body(sizes, pair, *rest):
    ny, nx, nz = sizes
    hidden = rest[-1].shape[0]
    tile_rows, tile_cols, _ = pair.shape
    fits = (
        ny == 4
        and hidden % (nx * nz * CHUNKS) == 0
        and nx * nz * tile_rows == ny * tile_cols
        and tile_rows % ROWS == 0
        and tile_cols % 128 == 0
        and 2 * 5 * hidden * tile_rows * tile_cols * 2 <= 48 * 2**20
    )
    return channel_body(sizes, pair, *rest) if fits else gather_body(pair, *rest)


def solution(mesh):
    in_specs = (P(("grp", "gx", "gz"), "gy", None), P("grp"), P(), P(), P(), P(), P(), P(), P())
    out_specs = P(("grp", "gx", "gz"), "gy", None)
    sizes = (mesh.shape["gy"], mesh.shape["gx"], mesh.shape["gz"])
    return jax.shard_map(
        functools.partial(body, sizes), mesh=mesh, in_specs=in_specs, out_specs=out_specs, check_vma=False
    )
```

```python
import functools

import jax
import jax.numpy as jnp
from jax import lax
from jax.experimental import pallas as pl
from jax.experimental.pallas import tpu as pltpu
from jax.sharding import PartitionSpec as P

CHUNKS = 32
LAG = 2
ROWS = 16


def layer_norm(values, gain, bias):
    values = values.astype(jnp.float32)
    mean = jnp.mean(values, -1, keepdims=True)
    spread = jnp.mean(jnp.square(values - mean), -1, keepdims=True)
    return (values - mean) * lax.rsqrt(spread + 1e-05) * gain + bias


def channel_norm(values, gain, bias):
    mean = jnp.mean(values, 0, keepdims=True)
    spread = jnp.mean(jnp.square(values - mean), 0, keepdims=True)
    return (values - mean) * lax.rsqrt(spread + 1e-05) * gain[:, None, None] + bias[:, None, None]


def gather_body(pair, lengths, ln_gain, ln_bias, w_ab, w_gate, out_gain, out_bias, w_out):
    tile_rows, tile_cols, width = pair.shape
    hidden = w_out.shape[0]
    row_start = lax.axis_index(("gx", "gz")) * tile_rows
    col_index = lax.axis_index("gy")
    col_start = col_index * tile_cols
    normed = layer_norm(pair, ln_gain, ln_bias).astype(jnp.bfloat16)
    flat = normed.reshape(tile_rows * tile_cols, width)
    proj = jnp.dot(flat, w_ab, preferred_element_type=jnp.float32).reshape(
        tile_rows, tile_cols, 4 * hidden
    )
    row_live = (row_start + jnp.arange(tile_rows, dtype=jnp.int32) < lengths[0]).astype(jnp.float32)
    col_live = (col_start + jnp.arange(tile_cols, dtype=jnp.int32) < lengths[0]).astype(jnp.float32)
    pair_mask = (row_live[:, None] * col_live[None, :])[..., None]
    left = (pair_mask * jax.nn.sigmoid(proj[..., :hidden]) * proj[..., hidden : 2 * hidden]).astype(
        jnp.bfloat16
    )
    right = (
        pair_mask * jax.nn.sigmoid(proj[..., 2 * hidden : 3 * hidden]) * proj[..., 3 * hidden :]
    ).astype(jnp.bfloat16)
    left_major = jnp.transpose(left, (2, 0, 1))
    right_major = jnp.transpose(right, (2, 0, 1))
    column_rows = lax.all_gather(right_major, ("gx", "gz"), axis=1, tiled=True)
    right_mine = lax.all_to_all(column_rows, "gy", split_axis=1, concat_axis=2, tiled=True)
    triangle = jnp.einsum(
        "cik,cjk->cij",
        lax.all_gather(left_major, "gy", axis=2, tiled=True),
        right_mine,
        preferred_element_type=jnp.float32,
    )
    tri_norm = channel_norm(triangle, out_gain, out_bias).astype(jnp.bfloat16)
    gate = jax.nn.sigmoid(jnp.dot(flat, w_gate, preferred_element_type=jnp.float32)).reshape(
        tile_rows, tile_cols, width
    )
    projected = jnp.einsum("cij,cd->ijd", tri_norm, w_out, preferred_element_type=jnp.float32)
    return (gate * projected).astype(jnp.bfloat16)


def project_kernel(nz, lengths, pair, gain, bias, w_ab, out):
    rows, cols, width = pair.shape
    hidden = out.shape[1]
    flat = pair[...].reshape(rows * cols, width)
    normed = layer_norm(flat, gain[...], bias[...]).astype(jnp.bfloat16)
    proj = lax.dot_general(
        w_ab[...], normed, (((0,), (1,)), ((), ())), preferred_element_type=jnp.float32
    )
    lane = lax.broadcasted_iota(jnp.int32, (1, rows * cols), 1)
    block = (lax.axis_index("gx") * nz + lax.axis_index("gz")) * pl.num_programs(0)
    row = (block + pl.program_id(0)) * rows + lane // cols
    col = lax.axis_index("gy") * cols + lane % cols
    mask = ((row < lengths[0]) & (col < lengths[0])).astype(jnp.float32)
    for side in range(2):
        base = 2 * side * hidden
        value = (
            mask * jax.nn.sigmoid(proj[base : base + hidden]) * proj[base + hidden : base + 2 * hidden]
        )
        out[side] = value.reshape(hidden, rows, cols).astype(jnp.bfloat16)


def exchange_kernel(
    nx,
    nz,
    send,
    out,
    held,
    given,
    taken,
    deal_send,
    deal_recv,
    pass_send,
    pass_recv,
    cross_send,
    cross_recv,
    back_send,
    back_recv,
    own_sem,
):
    nr = nx * nz
    hidden, rows, cols = send.shape[1:]
    each = hidden // nr
    chunks = pass_send.shape[0]
    part = each // chunks
    gy, gx, gz = lax.axis_index("gy"), lax.axis_index("gx"), lax.axis_index("gz")
    me = gx * nz + gz
    half = gy // 2
    inner_plane, outer_plane = 1 + half, 3 * half
    inner = gy == inner_plane

    def place(tall, plane):
        return {"gy": plane, "gx": tall // nz, "gz": tall % nz}

    def remote(src, dst, send_sem, recv_sem, device):
        return pltpu.make_async_remote_copy(
            src_ref=src,
            dst_ref=dst,
            send_sem=send_sem,
            recv_sem=recv_sem,
            device_id=device,
            device_id_type=pl.DeviceIdType.MESH,
        )

    def channels(chunk):
        return pl.ds(chunk * part, part)

    def band(tall):
        return pl.ds(pl.multiple_of(tall * rows, rows), rows)

    def columns(plane):
        return pl.ds(pl.multiple_of((plane - 2 * half) * cols, cols), cols)

    def deal(chunk, step):
        peer = lax.rem(me + step, nr)
        return remote(
            send.at[:, pl.ds(peer * each + chunk * part, part)],
            held.at[:, channels(chunk), band(me), pl.ds(0, cols)],
            deal_send.at[chunk, step],
            deal_recv.at[chunk, step],
            place(peer, gy),
        )

    def keep_in(chunk):
        return pltpu.make_async_copy(
            send.at[:, pl.ds(me * each + chunk * part, part)],
            held.at[:, channels(chunk), band(me), pl.ds(0, cols)],
            own_sem.at[0, chunk],
        )

    def pass_on(chunk):
        return remote(
            held.at[:, channels(chunk), :, pl.ds(0, cols)],
            held.at[:, channels(chunk), :, pl.ds(cols, cols)],
            pass_send.at[chunk],
            pass_recv.at[chunk],
            place(me, inner_plane),
        )

    def cross(chunk):
        return remote(
            given.at[channels(chunk)],
            taken.at[channels(chunk)],
            cross_send.at[chunk],
            cross_recv.at[chunk],
            place(me, 3 - gy),
        )

    def hand_back(chunk, step, plane, side):
        peer = lax.rem(me + step, nr)
        return remote(
            taken.at[channels(chunk), band(peer), columns(plane)],
            out.at[pl.ds(me * each + chunk * part, part)],
            back_send.at[side, chunk, step],
            back_recv.at[chunk, step],
            place(peer, plane),
        )

    def keep_out(chunk):
        return pltpu.make_async_copy(
            taken.at[channels(chunk), band(me), columns(inner_plane)],
            out.at[pl.ds(me * each + chunk * part, part)],
            own_sem.at[1, chunk],
        )

    barrier = pltpu.get_barrier_semaphore()
    total = 4 * nr
    index = gy * nr + me
    for step in range(1, total):
        peer = lax.rem(index + step, total)
        pl.semaphore_signal(
            barrier,
            inc=1,
            device_id=place(peer % nr, peer // nr),
            device_id_type=pl.DeviceIdType.MESH,
        )
    pl.semaphore_wait(barrier, total - 1)

    @pl.loop(0, chunks)
    def _(chunk):
        for step in range(1, nr):
            deal(chunk, step).start()
        keep_in(chunk).start()

    def dealt(chunk):
        for step in range(1, nr):
            deal(chunk, step).wait_recv()
        keep_in(chunk).wait()

    def product(channel, which):
        below = pl.ds(pl.multiple_of(which * 2 * cols, 2 * cols), 2 * cols)
        return lax.dot_general(
            held[0, channel],
            held[1, channel, below, :],
            (((1,), (1,)), ((), ())),
            preferred_element_type=jnp.float32,
        )

    @pl.when(jnp.logical_not(inner))
    def _():
        @pl.loop(0, chunks)
        def _(chunk):
            dealt(chunk)
            pass_on(chunk).start()

        @pl.loop(0, chunks)
        def _(chunk):
            for step in range(nr):
                hand_back(chunk, step, outer_plane, 1).wait_recv()
            for step in range(1, nr):
                deal(chunk, step).wait_send()
            pass_on(chunk).wait_send()

    @pl.when(inner)
    def _():
        @pl.loop(0, chunks + LAG)
        def _(turn):
            @pl.when(turn < chunks)
            def _():
                dealt(turn)
                pass_on(turn).wait_recv()

                @pl.loop(turn * part, (turn + 1) * part)
                def _(channel):
                    given[channel] = product(channel, 1 - half).astype(jnp.bfloat16)

                cross(turn).start()

            @pl.when(turn >= LAG)
            def _():
                chunk = turn - LAG
                cross(chunk).wait_recv()

                @pl.loop(chunk * part, (chunk + 1) * part)
                def _(channel):
                    total = product(channel, half) + taken[channel].astype(jnp.float32)
                    taken[channel] = total.astype(jnp.bfloat16)

                for step in range(nr):
                    hand_back(chunk, step, outer_plane, 1).start()
                for step in range(1, nr):
                    hand_back(chunk, step, inner_plane, 0).start()
                keep_out(chunk).start()

        @pl.loop(0, chunks)
        def _(chunk):
            for step in range(1, nr):
                hand_back(chunk, step, inner_plane, 0).wait_recv()
                hand_back(chunk, step, inner_plane, 0).wait_send()
                deal(chunk, step).wait_send()
            for step in range(nr):
                hand_back(chunk, step, outer_plane, 1).wait_send()
            cross(chunk).wait_send()
            keep_out(chunk).wait()


def upright(row):
    return jnp.transpose(jnp.broadcast_to(row[...], (row.shape[1], row.shape[1])))[:, :1]


def finish_kernel(pair, tri, gain, bias, w_gate, out_gain, out_bias, w_out, out):
    rows, cols, width = pair.shape
    hidden = tri.shape[0]
    flat = pair[...].reshape(rows * cols, width)
    normed = layer_norm(flat, gain[...], bias[...]).astype(jnp.bfloat16)
    gate = jax.nn.sigmoid(jnp.dot(normed, w_gate[...], preferred_element_type=jnp.float32))
    values = tri[...].astype(jnp.float32)
    mean = jnp.mean(values, 0, keepdims=True)
    centred = values - mean
    spread = jnp.mean(jnp.square(centred), 0, keepdims=True)
    scaled = (centred * lax.rsqrt(spread + 1e-05)).reshape(hidden, rows * cols)
    tri_norm = (scaled * upright(out_gain) + upright(out_bias)).astype(jnp.bfloat16)
    projected = lax.dot_general(
        tri_norm, w_out[...], (((0,), (0,)), ((), ())), preferred_element_type=jnp.float32
    )
    out[...] = (gate * projected).astype(jnp.bfloat16).reshape(rows, cols, width)


def whole(shape):
    return pl.BlockSpec(shape, lambda step: (0,) * len(shape))


def channel_body(sizes, pair, lengths, ln_gain, ln_bias, w_ab, w_gate, out_gain, out_bias, w_out):
    ny, nx, nz = sizes
    tile_rows, tile_cols, width = pair.shape
    hidden = w_out.shape[0]
    gain, bias = ln_gain[None, :], ln_bias[None, :]
    smem = pl.BlockSpec(memory_space=pltpu.SMEM)
    steps = tile_rows // ROWS
    sides = pl.pallas_call(
        functools.partial(project_kernel, nz),
        name="project",
        grid=(steps,),
        out_shape=jax.ShapeDtypeStruct((2, hidden, tile_rows, tile_cols), jnp.bfloat16),
        in_specs=[
            smem,
            pl.BlockSpec((ROWS, tile_cols, width), lambda step: (step, 0, 0)),
            whole((1, width)),
            whole((1, width)),
            whole((width, 4 * hidden)),
        ],
        out_specs=pl.BlockSpec((2, hidden, ROWS, tile_cols), lambda step: (0, 0, step, 0)),
        compiler_params=pltpu.CompilerParams(vmem_limit_bytes=56 * 2**20),
    )(lengths, pair, gain, bias, w_ab)
    dma = pltpu.SemaphoreType.DMA
    any_space = pl.BlockSpec(memory_space=pl.ANY)
    nr = nx * nz
    each, side = hidden // nr, nr * tile_rows
    triangle = pl.pallas_call(
        functools.partial(exchange_kernel, nx, nz),
        name="exchange",
        out_shape=jax.ShapeDtypeStruct((hidden, tile_rows, tile_cols), jnp.bfloat16),
        in_specs=[any_space],
        out_specs=any_space,
        scratch_shapes=[
            pltpu.VMEM((2, each, side, 2 * tile_cols), jnp.bfloat16),
            pltpu.VMEM((each, side, 2 * tile_cols), jnp.bfloat16),
            pltpu.VMEM((each, side, 2 * tile_cols), jnp.bfloat16),
            dma((CHUNKS, nr)),
            dma((CHUNKS, nr)),
            dma((CHUNKS,)),
            dma((CHUNKS,)),
            dma((CHUNKS,)),
            dma((CHUNKS,)),
            dma((2, CHUNKS, nr)),
            dma((CHUNKS, nr)),
            dma((2, CHUNKS)),
        ],
        compiler_params=pltpu.CompilerParams(
            collective_id=0, has_side_effects=True, vmem_limit_bytes=56 * 2**20
        ),
    )(sides)
    return pl.pallas_call(
        finish_kernel,
        name="finish",
        grid=(steps,),
        out_shape=jax.ShapeDtypeStruct(pair.shape, jnp.bfloat16),
        in_specs=[
            pl.BlockSpec((ROWS, tile_cols, width), lambda step: (step, 0, 0)),
            pl.BlockSpec((hidden, ROWS, tile_cols), lambda step: (0, step, 0)),
            whole((1, width)),
            whole((1, width)),
            whole((width, width)),
            whole((1, hidden)),
            whole((1, hidden)),
            whole((hidden, width)),
        ],
        out_specs=pl.BlockSpec((ROWS, tile_cols, width), lambda step: (step, 0, 0)),
        compiler_params=pltpu.CompilerParams(vmem_limit_bytes=56 * 2**20),
    )(pair, triangle, gain, bias, w_gate, out_gain[None, :], out_bias[None, :], w_out)


def body(sizes, pair, *rest):
    ny, nx, nz = sizes
    hidden = rest[-1].shape[0]
    tile_rows, tile_cols, _ = pair.shape
    fits = (
        ny == 4
        and hidden % (nx * nz * CHUNKS) == 0
        and nx * nz * tile_rows == ny * tile_cols
        and tile_rows % ROWS == 0
        and tile_cols % 128 == 0
        and 2 * 5 * hidden * tile_rows * tile_cols * 2 <= 48 * 2**20
    )
    return channel_body(sizes, pair, *rest) if fits else gather_body(pair, *rest)


def solution(mesh):
    in_specs = (P(("grp", "gx", "gz"), "gy", None), P("grp"), P(), P(), P(), P(), P(), P(), P())
    out_specs = P(("grp", "gx", "gz"), "gy", None)
    sizes = (mesh.shape["gy"], mesh.shape["gx"], mesh.shape["gz"])
    return jax.shard_map(
        functools.partial(body, sizes), mesh=mesh, in_specs=in_specs, out_specs=out_specs, check_vma=False
    )
```

```python
import functools

import jax
import jax.numpy as jnp
from jax import lax
from jax.experimental import pallas as pl
from jax.experimental.pallas import tpu as pltpu
from jax.sharding import PartitionSpec as P

CHUNKS = 32
LAG = 3
GROUPS = 4
ROWS = 16


def layer_norm(values, gain, bias):
    values = values.astype(jnp.float32)
    mean = jnp.mean(values, -1, keepdims=True)
    spread = jnp.mean(jnp.square(values - mean), -1, keepdims=True)
    return (values - mean) * lax.rsqrt(spread + 1e-05) * gain + bias


def channel_norm(values, gain, bias):
    mean = jnp.mean(values, 0, keepdims=True)
    spread = jnp.mean(jnp.square(values - mean), 0, keepdims=True)
    return (values - mean) * lax.rsqrt(spread + 1e-05) * gain[:, None, None] + bias[:, None, None]


def gather_body(pair, lengths, ln_gain, ln_bias, w_ab, w_gate, out_gain, out_bias, w_out):
    tile_rows, tile_cols, width = pair.shape
    hidden = w_out.shape[0]
    row_start = lax.axis_index(("gx", "gz")) * tile_rows
    col_index = lax.axis_index("gy")
    col_start = col_index * tile_cols
    normed = layer_norm(pair, ln_gain, ln_bias).astype(jnp.bfloat16)
    flat = normed.reshape(tile_rows * tile_cols, width)
    proj = jnp.dot(flat, w_ab, preferred_element_type=jnp.float32).reshape(
        tile_rows, tile_cols, 4 * hidden
    )
    row_live = (row_start + jnp.arange(tile_rows, dtype=jnp.int32) < lengths[0]).astype(jnp.float32)
    col_live = (col_start + jnp.arange(tile_cols, dtype=jnp.int32) < lengths[0]).astype(jnp.float32)
    pair_mask = (row_live[:, None] * col_live[None, :])[..., None]
    left = (pair_mask * jax.nn.sigmoid(proj[..., :hidden]) * proj[..., hidden : 2 * hidden]).astype(
        jnp.bfloat16
    )
    right = (
        pair_mask * jax.nn.sigmoid(proj[..., 2 * hidden : 3 * hidden]) * proj[..., 3 * hidden :]
    ).astype(jnp.bfloat16)
    left_major = jnp.transpose(left, (2, 0, 1))
    right_major = jnp.transpose(right, (2, 0, 1))
    column_rows = lax.all_gather(right_major, ("gx", "gz"), axis=1, tiled=True)
    right_mine = lax.all_to_all(column_rows, "gy", split_axis=1, concat_axis=2, tiled=True)
    triangle = jnp.einsum(
        "cik,cjk->cij",
        lax.all_gather(left_major, "gy", axis=2, tiled=True),
        right_mine,
        preferred_element_type=jnp.float32,
    )
    tri_norm = channel_norm(triangle, out_gain, out_bias).astype(jnp.bfloat16)
    gate = jax.nn.sigmoid(jnp.dot(flat, w_gate, preferred_element_type=jnp.float32)).reshape(
        tile_rows, tile_cols, width
    )
    projected = jnp.einsum("cij,cd->ijd", tri_norm, w_out, preferred_element_type=jnp.float32)
    return (gate * projected).astype(jnp.bfloat16)


def exchange_kernel(
    nx,
    nz,
    lengths,
    pair,
    gain,
    bias,
    w_ab,
    w_gate,
    out,
    gate_out,
    normed,
    send,
    gate_held,
    held,
    given,
    taken,
    deal_send,
    deal_recv,
    pass_send,
    pass_recv,
    cross_send,
    cross_recv,
    back_send,
    back_recv,
    own_sem,
    pair_sem,
    gate_sem,
):
    nr = nx * nz
    hidden, rows, cols = send.shape[1:]
    width = pair.shape[2]
    blocks, lanes = rows // ROWS, ROWS * cols
    each = hidden // nr
    chunks = pass_send.shape[0]
    part = each // chunks
    gy, gx, gz = lax.axis_index("gy"), lax.axis_index("gx"), lax.axis_index("gz")
    me = gx * nz + gz
    half = gy // 2
    inner_plane, outer_plane = 1 + half, 3 * half
    inner = gy == inner_plane

    def place(tall, plane):
        return {"gy": plane, "gx": tall // nz, "gz": tall % nz}

    def remote(src, dst, send_sem, recv_sem, device):
        return pltpu.make_async_remote_copy(
            src_ref=src,
            dst_ref=dst,
            send_sem=send_sem,
            recv_sem=recv_sem,
            device_id=device,
            device_id_type=pl.DeviceIdType.MESH,
        )

    def channels(chunk):
        return pl.ds(chunk * part, part)

    def band(tall):
        return pl.ds(pl.multiple_of(tall * rows, rows), rows)

    def columns(plane):
        return pl.ds(pl.multiple_of((plane - 2 * half) * cols, cols), cols)

    def deal(chunk, step):
        peer = lax.rem(me + step, nr)
        return remote(
            send.at[:, pl.ds(peer * each + chunk * part, part)],
            held.at[:, channels(chunk), band(me), pl.ds(0, cols)],
            deal_send.at[chunk, step],
            deal_recv.at[chunk, step],
            place(peer, gy),
        )

    def keep_in(chunk):
        return pltpu.make_async_copy(
            send.at[:, pl.ds(me * each + chunk * part, part)],
            held.at[:, channels(chunk), band(me), pl.ds(0, cols)],
            own_sem.at[0, chunk],
        )

    def pass_on(chunk):
        return remote(
            held.at[:, channels(chunk), :, pl.ds(0, cols)],
            held.at[:, channels(chunk), :, pl.ds(cols, cols)],
            pass_send.at[chunk],
            pass_recv.at[chunk],
            place(me, inner_plane),
        )

    def cross(chunk):
        return remote(
            given.at[channels(chunk)],
            taken.at[channels(chunk)],
            cross_send.at[chunk],
            cross_recv.at[chunk],
            place(me, 3 - gy),
        )

    def hand_back(chunk, step, plane, side):
        peer = lax.rem(me + step, nr)
        return remote(
            taken.at[channels(chunk), band(peer), columns(plane)],
            out.at[pl.ds(me * each + chunk * part, part)],
            back_send.at[side, chunk, step],
            back_recv.at[chunk, step],
            place(peer, plane),
        )

    def keep_out(chunk):
        return pltpu.make_async_copy(
            taken.at[channels(chunk), band(me), columns(inner_plane)],
            out.at[pl.ds(me * each + chunk * part, part)],
            own_sem.at[1, chunk],
        )

    def load(block):
        return pltpu.make_async_copy(
            pair.at[pl.ds(block * ROWS, ROWS)],
            normed.at[pl.ds(block * ROWS, ROWS)],
            pair_sem.at[block],
        )

    for block in range(blocks):
        load(block).start()
    barrier = pltpu.get_barrier_semaphore()
    total = 4 * nr
    index = gy * nr + me
    for step in range(1, total):
        peer = lax.rem(index + step, total)
        pl.semaphore_signal(
            barrier,
            inc=1,
            device_id=place(peer % nr, peer // nr),
            device_id_type=pl.DeviceIdType.MESH,
        )
    pl.semaphore_wait(barrier, total - 1)

    def dealt(chunk):
        for step in range(1, nr):
            deal(chunk, step).wait_recv()
        keep_in(chunk).wait()

    def product(channel, which):
        below = pl.ds(pl.multiple_of(which * 2 * cols, 2 * cols), 2 * cols)
        return lax.dot_general(
            held[0, channel],
            held[1, channel, below, :],
            (((1,), (1,)), ((), ())),
            preferred_element_type=jnp.float32,
        )

    @pl.loop(0, blocks)
    def _(block):
        load(block).wait()
        here = pl.ds(pl.multiple_of(block * ROWS, ROWS), ROWS)
        flat = normed[here].reshape(lanes, width)
        value = layer_norm(flat, gain[...], bias[...]).astype(jnp.bfloat16)
        normed[here] = value.reshape(ROWS, cols, width)

    upright_w = jnp.transpose(w_ab[...].astype(jnp.float32))
    lane = lax.broadcasted_iota(jnp.int32, (1, lanes), 1)
    col_live = gy * cols + lane % cols < lengths[0]
    span = each // GROUPS

    def project(group):
        starts = [
            kind * hidden + tall * each + group * span for kind in range(4) for tall in range(nr)
        ]
        weights = jnp.concatenate([upright_w[at : at + span] for at in starts]).astype(jnp.bfloat16)
        height = nr * span

        @pl.loop(0, blocks)
        def _(block):
            here = pl.ds(pl.multiple_of(block * ROWS, ROWS), ROWS)
            proj = lax.dot_general(
                weights,
                normed[here].reshape(lanes, width),
                (((1,), (1,)), ((), ())),
                preferred_element_type=jnp.float32,
            )
            row_live = me * rows + block * ROWS + lane // cols < lengths[0]
            mask = (row_live & col_live).astype(jnp.float32)
            for side in range(2):
                gates = proj[2 * side * height : (2 * side + 1) * height]
                values = proj[(2 * side + 1) * height : (2 * side + 2) * height]
                value = mask * jax.nn.sigmoid(gates) * values
                value = value.reshape(height, ROWS, cols).astype(jnp.bfloat16)
                for tall in range(nr):
                    first = tall * each + group * span
                    send[side, first : first + span, here] = value[tall * span : (tall + 1) * span]

        @pl.loop(group * span // part, (group + 1) * span // part)
        def _(chunk):
            for step in range(1, nr):
                deal(chunk, step).start()
            keep_in(chunk).start()

    outer = jnp.logical_not(inner)
    for group in range(GROUPS):
        project(group)
        if group:

            @pl.when(outer)
            def _():
                dealt(group - 1)
                pass_on(group - 1).start()

    def store_gate(block):
        return pltpu.make_async_copy(
            gate_held.at[block % 2],
            gate_out.at[pl.ds(block * ROWS, ROWS)],
            gate_sem.at[block % 2],
        )

    def gate_turn(turn):
        block = turn - 2 * GROUPS

        @pl.when((block >= 2) & (block < blocks + 2))
        def _():
            store_gate(block - 2).wait()

        @pl.when((block >= 0) & (block < blocks))
        def _():
            here = pl.ds(pl.multiple_of(block * ROWS, ROWS), ROWS)
            value = jax.nn.sigmoid(
                jnp.dot(
                    normed[here].reshape(lanes, width),
                    w_gate[...],
                    preferred_element_type=jnp.float32,
                )
            )
            gate_held[block % 2] = value.reshape(ROWS, cols, width)
            store_gate(block).start()

    @pl.when(outer)
    def _():
        @pl.loop(GROUPS - 1, chunks)
        def _(chunk):
            dealt(chunk)
            pass_on(chunk).start()
            gate_turn(chunk)

        @pl.loop(0, chunks)
        def _(chunk):
            for step in range(nr):
                hand_back(chunk, step, outer_plane, 1).wait_recv()
            for step in range(1, nr):
                deal(chunk, step).wait_send()
            pass_on(chunk).wait_send()

    @pl.when(inner)
    def _():
        @pl.loop(0, chunks + LAG)
        def _(turn):
            @pl.when(turn < chunks)
            def _():
                dealt(turn)
                pass_on(turn).wait_recv()

                @pl.loop(turn * part, (turn + 1) * part)
                def _(channel):
                    given[channel] = product(channel, 1 - half).astype(jnp.bfloat16)

                cross(turn).start()

            @pl.when(turn >= LAG)
            def _():
                chunk = turn - LAG
                cross(chunk).wait_recv()

                @pl.loop(chunk * part, (chunk + 1) * part)
                def _(channel):
                    total = product(channel, half) + taken[channel].astype(jnp.float32)
                    taken[channel] = total.astype(jnp.bfloat16)

                for step in range(nr):
                    hand_back(chunk, step, outer_plane, 1).start()
                for step in range(1, nr):
                    hand_back(chunk, step, inner_plane, 0).start()
                keep_out(chunk).start()

            gate_turn(turn)

        @pl.loop(0, chunks)
        def _(chunk):
            for step in range(1, nr):
                hand_back(chunk, step, inner_plane, 0).wait_recv()
                hand_back(chunk, step, inner_plane, 0).wait_send()
                deal(chunk, step).wait_send()
            for step in range(nr):
                hand_back(chunk, step, outer_plane, 1).wait_send()
            cross(chunk).wait_send()
            keep_out(chunk).wait()


def upright(row):
    return jnp.transpose(jnp.broadcast_to(row[...], (row.shape[1], row.shape[1])))[:, :1]


def finish_kernel(gate, tri, out_gain, out_bias, w_out, out):
    rows, cols, width = out.shape
    hidden = tri.shape[0]
    values = tri[...].astype(jnp.float32)
    mean = jnp.mean(values, 0, keepdims=True)
    centred = values - mean
    spread = jnp.mean(jnp.square(centred), 0, keepdims=True)
    scaled = (centred * lax.rsqrt(spread + 1e-05)).reshape(hidden, rows * cols)
    tri_norm = (scaled * upright(out_gain) + upright(out_bias)).astype(jnp.bfloat16)
    projected = lax.dot_general(
        tri_norm, w_out[...], (((0,), (0,)), ((), ())), preferred_element_type=jnp.float32
    )
    out[...] = (gate[...] * projected.reshape(rows, cols, width)).astype(jnp.bfloat16)


def whole(shape):
    return pl.BlockSpec(shape, lambda step: (0,) * len(shape))


def channel_body(sizes, pair, lengths, ln_gain, ln_bias, w_ab, w_gate, out_gain, out_bias, w_out):
    ny, nx, nz = sizes
    tile_rows, tile_cols, width = pair.shape
    hidden = w_out.shape[0]
    gain, bias = ln_gain[None, :], ln_bias[None, :]
    smem = pl.BlockSpec(memory_space=pltpu.SMEM)
    steps = tile_rows // ROWS
    dma = pltpu.SemaphoreType.DMA
    any_space = pl.BlockSpec(memory_space=pl.ANY)
    nr = nx * nz
    each, side = hidden // nr, nr * tile_rows
    vmem = pl.BlockSpec(memory_space=pltpu.VMEM)
    triangle, gate = pl.pallas_call(
        functools.partial(exchange_kernel, nx, nz),
        name="exchange",
        out_shape=(
            jax.ShapeDtypeStruct((hidden, tile_rows, tile_cols), jnp.bfloat16),
            jax.ShapeDtypeStruct(pair.shape, jnp.float32),
        ),
        in_specs=[smem, any_space, vmem, vmem, vmem, vmem],
        out_specs=(any_space, any_space),
        scratch_shapes=[
            pltpu.VMEM(pair.shape, jnp.bfloat16),
            pltpu.VMEM((2, hidden, tile_rows, tile_cols), jnp.bfloat16),
            pltpu.VMEM((2, ROWS, tile_cols, width), jnp.float32),
            pltpu.VMEM((2, each, side, 2 * tile_cols), jnp.bfloat16),
            pltpu.VMEM((each, side, 2 * tile_cols), jnp.bfloat16),
            pltpu.VMEM((each, side, 2 * tile_cols), jnp.bfloat16),
            dma((CHUNKS, nr)),
            dma((CHUNKS, nr)),
            dma((CHUNKS,)),
            dma((CHUNKS,)),
            dma((CHUNKS,)),
            dma((CHUNKS,)),
            dma((2, CHUNKS, nr)),
            dma((CHUNKS, nr)),
            dma((2, CHUNKS)),
            dma((steps,)),
            dma((2,)),
        ],
        compiler_params=pltpu.CompilerParams(
            collective_id=0, has_side_effects=True, vmem_limit_bytes=63 * 2**20
        ),
    )(lengths, pair, gain, bias, w_ab, w_gate)
    return pl.pallas_call(
        finish_kernel,
        name="finish",
        grid=(steps,),
        out_shape=jax.ShapeDtypeStruct(pair.shape, jnp.bfloat16),
        in_specs=[
            pl.BlockSpec((ROWS, tile_cols, width), lambda step: (step, 0, 0)),
            pl.BlockSpec((hidden, ROWS, tile_cols), lambda step: (0, step, 0)),
            whole((1, hidden)),
            whole((1, hidden)),
            whole((hidden, width)),
        ],
        out_specs=pl.BlockSpec((ROWS, tile_cols, width), lambda step: (step, 0, 0)),
        compiler_params=pltpu.CompilerParams(vmem_limit_bytes=56 * 2**20),
    )(gate, triangle, out_gain[None, :], out_bias[None, :], w_out)


def body(sizes, pair, *rest):
    ny, nx, nz = sizes
    hidden = rest[-1].shape[0]
    tile_rows, tile_cols, _ = pair.shape
    fits = (
        ny == 4
        and hidden % (nx * nz * CHUNKS) == 0
        and hidden % (nx * nz * GROUPS * 8) == 0
        and nx * nz * tile_rows == ny * tile_cols
        and tile_rows % ROWS == 0
        and tile_cols % 128 == 0
        and 2 * 5 * hidden * tile_rows * tile_cols * 2 <= 48 * 2**20
    )
    return channel_body(sizes, pair, *rest) if fits else gather_body(pair, *rest)


def solution(mesh):
    in_specs = (P(("grp", "gx", "gz"), "gy", None), P("grp"), P(), P(), P(), P(), P(), P(), P())
    out_specs = P(("grp", "gx", "gz"), "gy", None)
    sizes = (mesh.shape["gy"], mesh.shape["gx"], mesh.shape["gz"])
    return jax.shard_map(
        functools.partial(body, sizes), mesh=mesh, in_specs=in_specs, out_specs=out_specs, check_vma=False
    )
```

```python
import functools

import jax
import jax.numpy as jnp
from jax import lax
from jax.experimental import pallas as pl
from jax.experimental.pallas import tpu as pltpu
from jax.sharding import PartitionSpec as P

CHUNKS = 32
LAG = 2
GROUPS = 4
ROWS = 32


def layer_norm(values, gain, bias):
    values = values.astype(jnp.float32)
    mean = jnp.mean(values, -1, keepdims=True)
    spread = jnp.mean(jnp.square(values - mean), -1, keepdims=True)
    return (values - mean) * lax.rsqrt(spread + 1e-05) * gain + bias


def channel_norm(values, gain, bias):
    mean = jnp.mean(values, 0, keepdims=True)
    spread = jnp.mean(jnp.square(values - mean), 0, keepdims=True)
    return (values - mean) * lax.rsqrt(spread + 1e-05) * gain[:, None, None] + bias[:, None, None]


def gather_body(pair, lengths, ln_gain, ln_bias, w_ab, w_gate, out_gain, out_bias, w_out):
    tile_rows, tile_cols, width = pair.shape
    hidden = w_out.shape[0]
    row_start = lax.axis_index(("gx", "gz")) * tile_rows
    col_index = lax.axis_index("gy")
    col_start = col_index * tile_cols
    normed = layer_norm(pair, ln_gain, ln_bias).astype(jnp.bfloat16)
    flat = normed.reshape(tile_rows * tile_cols, width)
    proj = jnp.dot(flat, w_ab, preferred_element_type=jnp.float32).reshape(
        tile_rows, tile_cols, 4 * hidden
    )
    row_live = (row_start + jnp.arange(tile_rows, dtype=jnp.int32) < lengths[0]).astype(jnp.float32)
    col_live = (col_start + jnp.arange(tile_cols, dtype=jnp.int32) < lengths[0]).astype(jnp.float32)
    pair_mask = (row_live[:, None] * col_live[None, :])[..., None]
    left = (pair_mask * jax.nn.sigmoid(proj[..., :hidden]) * proj[..., hidden : 2 * hidden]).astype(
        jnp.bfloat16
    )
    right = (
        pair_mask * jax.nn.sigmoid(proj[..., 2 * hidden : 3 * hidden]) * proj[..., 3 * hidden :]
    ).astype(jnp.bfloat16)
    left_major = jnp.transpose(left, (2, 0, 1))
    right_major = jnp.transpose(right, (2, 0, 1))
    column_rows = lax.all_gather(right_major, ("gx", "gz"), axis=1, tiled=True)
    right_mine = lax.all_to_all(column_rows, "gy", split_axis=1, concat_axis=2, tiled=True)
    triangle = jnp.einsum(
        "cik,cjk->cij",
        lax.all_gather(left_major, "gy", axis=2, tiled=True),
        right_mine,
        preferred_element_type=jnp.float32,
    )
    tri_norm = channel_norm(triangle, out_gain, out_bias).astype(jnp.bfloat16)
    gate = jax.nn.sigmoid(jnp.dot(flat, w_gate, preferred_element_type=jnp.float32)).reshape(
        tile_rows, tile_cols, width
    )
    projected = jnp.einsum("cij,cd->ijd", tri_norm, w_out, preferred_element_type=jnp.float32)
    return (gate * projected).astype(jnp.bfloat16)


def exchange_kernel(
    nx,
    nz,
    lengths,
    pair,
    gain,
    bias,
    w_ab,
    w_gate,
    out,
    gate_out,
    normed,
    send,
    gate_held,
    held,
    given,
    taken,
    deal_send,
    deal_recv,
    pass_send,
    pass_recv,
    cross_send,
    cross_recv,
    back_send,
    back_recv,
    own_sem,
    pair_sem,
    gate_sem,
):
    nr = nx * nz
    hidden, rows, cols = send.shape[1:]
    width = pair.shape[2]
    blocks, lanes = rows // ROWS, ROWS * cols
    each = hidden // nr
    chunks = pass_send.shape[0]
    part = each // chunks
    gy, gx, gz = lax.axis_index("gy"), lax.axis_index("gx"), lax.axis_index("gz")
    me = gx * nz + gz
    half = gy // 2
    inner_plane, outer_plane = 1 + half, 3 * half
    inner = gy == inner_plane
    outer = jnp.logical_not(inner)

    def place(tall, plane):
        return {"gy": plane, "gx": tall // nz, "gz": tall % nz}

    def remote(src, dst, send_sem, recv_sem, device):
        return pltpu.make_async_remote_copy(
            src_ref=src,
            dst_ref=dst,
            send_sem=send_sem,
            recv_sem=recv_sem,
            device_id=device,
            device_id_type=pl.DeviceIdType.MESH,
        )

    def channels(chunk):
        return pl.ds(chunk * part, part)

    def band(tall):
        return pl.ds(pl.multiple_of(tall * rows, rows), rows)

    def columns(plane):
        return pl.ds(pl.multiple_of((plane - 2 * half) * cols, cols), cols)

    def deal(chunk, step):
        peer = lax.rem(me + step, nr)
        return remote(
            send.at[:, pl.ds(peer * each + chunk * part, part)],
            held.at[:, channels(chunk), band(me), pl.ds(0, cols)],
            deal_send.at[chunk, step],
            deal_recv.at[chunk, step],
            place(peer, gy),
        )

    def keep_in(chunk):
        return pltpu.make_async_copy(
            send.at[:, pl.ds(me * each + chunk * part, part)],
            held.at[:, channels(chunk), band(me), pl.ds(0, cols)],
            own_sem.at[0, chunk],
        )

    def deal_inward(chunk, step):
        peer = lax.rem(me + step, nr)
        return remote(
            send.at[:, pl.ds(peer * each + chunk * part, part)],
            held.at[:, channels(chunk), band(me), pl.ds(cols, cols)],
            pass_send.at[chunk, step],
            pass_recv.at[chunk, step],
            place(peer, inner_plane),
        )

    def cross(chunk):
        return remote(
            given.at[channels(chunk)],
            taken.at[channels(chunk)],
            cross_send.at[chunk],
            cross_recv.at[chunk],
            place(me, 3 - gy),
        )

    def hand_back(chunk, step, plane, side):
        peer = lax.rem(me + step, nr)
        return remote(
            taken.at[channels(chunk), band(peer), columns(plane)],
            out.at[pl.ds(me * each + chunk * part, part)],
            back_send.at[side, chunk, step],
            back_recv.at[chunk, step],
            place(peer, plane),
        )

    def keep_out(chunk):
        return pltpu.make_async_copy(
            taken.at[channels(chunk), band(me), columns(inner_plane)],
            out.at[pl.ds(me * each + chunk * part, part)],
            own_sem.at[1, chunk],
        )

    def load(block):
        return pltpu.make_async_copy(
            pair.at[pl.ds(block * ROWS, ROWS)],
            normed.at[pl.ds(block * ROWS, ROWS)],
            pair_sem.at[block],
        )

    for block in range(blocks):
        load(block).start()
    barrier = pltpu.get_barrier_semaphore()
    total = 4 * nr
    index = gy * nr + me
    for step in range(1, total):
        peer = lax.rem(index + step, total)
        pl.semaphore_signal(
            barrier,
            inc=1,
            device_id=place(peer % nr, peer // nr),
            device_id_type=pl.DeviceIdType.MESH,
        )
    def dealt(chunk):
        for step in range(1, nr):
            deal(chunk, step).wait_recv()
        keep_in(chunk).wait()

    def product(channel, which):
        below = pl.ds(pl.multiple_of(which * 2 * cols, 2 * cols), 2 * cols)
        return lax.dot_general(
            held[0, channel],
            held[1, channel, below, :],
            (((1,), (1,)), ((), ())),
            preferred_element_type=jnp.float32,
        )

    @pl.loop(0, blocks)
    def _(block):
        load(block).wait()
        here = pl.ds(pl.multiple_of(block * ROWS, ROWS), ROWS)
        flat = normed[here].reshape(lanes, width)
        value = layer_norm(flat, gain[...], bias[...]).astype(jnp.bfloat16)
        normed[here] = value.reshape(ROWS, cols, width)

    upright_w = jnp.transpose(w_ab[...].astype(jnp.float32))
    lane = lax.broadcasted_iota(jnp.int32, (1, lanes), 1)
    col_live = gy * cols + lane % cols < lengths[0]
    span = each // GROUPS

    def project(group):
        starts = [
            kind * hidden + tall * each + group * span for kind in range(4) for tall in range(nr)
        ]
        weights = jnp.concatenate([upright_w[at : at + span] for at in starts]).astype(jnp.bfloat16)
        height = nr * span

        @pl.loop(0, blocks)
        def _(block):
            here = pl.ds(pl.multiple_of(block * ROWS, ROWS), ROWS)
            proj = lax.dot_general(
                weights,
                normed[here].reshape(lanes, width),
                (((1,), (1,)), ((), ())),
                preferred_element_type=jnp.float32,
            )
            row_live = me * rows + block * ROWS + lane // cols < lengths[0]
            mask = (row_live & col_live).astype(jnp.float32)
            for side in range(2):
                gates = proj[2 * side * height : (2 * side + 1) * height]
                values = proj[(2 * side + 1) * height : (2 * side + 2) * height]
                value = mask * jax.nn.sigmoid(gates) * values
                value = value.reshape(height, ROWS, cols).astype(jnp.bfloat16)
                for tall in range(nr):
                    first = tall * each + group * span
                    send[side, first : first + span, here] = value[tall * span : (tall + 1) * span]

        if group == 0:
            pl.semaphore_wait(barrier, total - 1)

        @pl.loop(group * span // part, (group + 1) * span // part)
        def _(chunk):
            @pl.when(inner)
            def _():
                for step in range(1, nr):
                    deal(chunk, step).start()
                keep_in(chunk).start()

            @pl.when(outer)
            def _():
                for step in range(nr):
                    deal_inward(chunk, step).start()

    for group in range(GROUPS):
        project(group)

    def store_gate(block):
        return pltpu.make_async_copy(
            gate_held.at[block % 2],
            gate_out.at[pl.ds(block * ROWS, ROWS)],
            gate_sem.at[block % 2],
        )

    def gate_turn(turn):
        block = turn - 2 * GROUPS

        @pl.when((block >= 2) & (block < blocks + 2))
        def _():
            store_gate(block - 2).wait()

        @pl.when((block >= 0) & (block < blocks))
        def _():
            here = pl.ds(pl.multiple_of(block * ROWS, ROWS), ROWS)
            value = jax.nn.sigmoid(
                jnp.dot(
                    normed[here].reshape(lanes, width),
                    w_gate[...],
                    preferred_element_type=jnp.float32,
                )
            )
            gate_held[block % 2] = value.reshape(ROWS, cols, width)
            store_gate(block).start()

    @pl.when(outer)
    def _():
        @pl.loop(0, chunks)
        def _(turn):
            gate_turn(turn)

        @pl.loop(0, chunks)
        def _(chunk):
            for step in range(nr):
                hand_back(chunk, step, outer_plane, 1).wait_recv()
                deal_inward(chunk, step).wait_send()

    @pl.when(inner)
    def _():
        @pl.loop(0, chunks + LAG)
        def _(turn):
            @pl.when(turn < chunks)
            def _():
                dealt(turn)
                for step in range(nr):
                    deal_inward(turn, step).wait_recv()

                @pl.loop(turn * part, (turn + 1) * part)
                def _(channel):
                    given[channel] = product(channel, 1 - half).astype(jnp.bfloat16)

                cross(turn).start()

            @pl.when(turn >= LAG)
            def _():
                chunk = turn - LAG
                cross(chunk).wait_recv()

                @pl.loop(chunk * part, (chunk + 1) * part)
                def _(channel):
                    total = product(channel, half) + taken[channel].astype(jnp.float32)
                    taken[channel] = total.astype(jnp.bfloat16)

                for step in range(nr):
                    hand_back(chunk, step, outer_plane, 1).start()
                for step in range(1, nr):
                    hand_back(chunk, step, inner_plane, 0).start()
                keep_out(chunk).start()

            gate_turn(turn)

        @pl.loop(0, chunks)
        def _(chunk):
            for step in range(1, nr):
                hand_back(chunk, step, inner_plane, 0).wait_recv()
                hand_back(chunk, step, inner_plane, 0).wait_send()
                deal(chunk, step).wait_send()
            for step in range(nr):
                hand_back(chunk, step, outer_plane, 1).wait_send()
            cross(chunk).wait_send()
            keep_out(chunk).wait()


def upright(row):
    return jnp.transpose(jnp.broadcast_to(row[...], (row.shape[1], row.shape[1])))[:, :1]


def finish_kernel(gate, tri, out_gain, out_bias, w_out, out):
    rows, cols, width = out.shape
    hidden = tri.shape[0]
    values = tri[...].astype(jnp.float32)
    mean = jnp.mean(values, 0, keepdims=True)
    centred = values - mean
    spread = jnp.mean(jnp.square(centred), 0, keepdims=True)
    scaled = (centred * lax.rsqrt(spread + 1e-05)).reshape(hidden, rows * cols)
    tri_norm = (scaled * upright(out_gain) + upright(out_bias)).astype(jnp.bfloat16)
    projected = lax.dot_general(
        tri_norm, w_out[...], (((0,), (0,)), ((), ())), preferred_element_type=jnp.float32
    )
    out[...] = (gate[...] * projected.reshape(rows, cols, width)).astype(jnp.bfloat16)


def whole(shape):
    return pl.BlockSpec(shape, lambda step: (0,) * len(shape))


def channel_body(sizes, pair, lengths, ln_gain, ln_bias, w_ab, w_gate, out_gain, out_bias, w_out):
    ny, nx, nz = sizes
    tile_rows, tile_cols, width = pair.shape
    hidden = w_out.shape[0]
    gain, bias = ln_gain[None, :], ln_bias[None, :]
    smem = pl.BlockSpec(memory_space=pltpu.SMEM)
    steps = tile_rows // ROWS
    dma = pltpu.SemaphoreType.DMA
    any_space = pl.BlockSpec(memory_space=pl.ANY)
    nr = nx * nz
    each, side = hidden // nr, nr * tile_rows
    vmem = pl.BlockSpec(memory_space=pltpu.VMEM)
    triangle, gate = pl.pallas_call(
        functools.partial(exchange_kernel, nx, nz),
        name="exchange",
        out_shape=(
            jax.ShapeDtypeStruct((hidden, tile_rows, tile_cols), jnp.bfloat16),
            jax.ShapeDtypeStruct(pair.shape, jnp.float32),
        ),
        in_specs=[smem, any_space, vmem, vmem, vmem, vmem],
        out_specs=(any_space, any_space),
        scratch_shapes=[
            pltpu.VMEM(pair.shape, jnp.bfloat16),
            pltpu.VMEM((2, hidden, tile_rows, tile_cols), jnp.bfloat16),
            pltpu.VMEM((2, ROWS, tile_cols, width), jnp.float32),
            pltpu.VMEM((2, each, side, 2 * tile_cols), jnp.bfloat16),
            pltpu.VMEM((each, side, 2 * tile_cols), jnp.bfloat16),
            pltpu.VMEM((each, side, 2 * tile_cols), jnp.bfloat16),
            dma((CHUNKS, nr)),
            dma((CHUNKS, nr)),
            dma((CHUNKS, nr)),
            dma((CHUNKS, nr)),
            dma((CHUNKS,)),
            dma((CHUNKS,)),
            dma((2, CHUNKS, nr)),
            dma((CHUNKS, nr)),
            dma((2, CHUNKS)),
            dma((steps,)),
            dma((2,)),
        ],
        compiler_params=pltpu.CompilerParams(
            collective_id=0, has_side_effects=True, vmem_limit_bytes=63 * 2**20
        ),
    )(lengths, pair, gain, bias, w_ab, w_gate)
    return pl.pallas_call(
        finish_kernel,
        name="finish",
        grid=(steps,),
        out_shape=jax.ShapeDtypeStruct(pair.shape, jnp.bfloat16),
        in_specs=[
            pl.BlockSpec((ROWS, tile_cols, width), lambda step: (step, 0, 0)),
            pl.BlockSpec((hidden, ROWS, tile_cols), lambda step: (0, step, 0)),
            whole((1, hidden)),
            whole((1, hidden)),
            whole((hidden, width)),
        ],
        out_specs=pl.BlockSpec((ROWS, tile_cols, width), lambda step: (step, 0, 0)),
        compiler_params=pltpu.CompilerParams(vmem_limit_bytes=56 * 2**20),
    )(gate, triangle, out_gain[None, :], out_bias[None, :], w_out)


def body(sizes, pair, *rest):
    ny, nx, nz = sizes
    hidden = rest[-1].shape[0]
    tile_rows, tile_cols, _ = pair.shape
    fits = (
        ny == 4
        and hidden % (nx * nz * CHUNKS) == 0
        and hidden % (nx * nz * GROUPS * 8) == 0
        and nx * nz * tile_rows == ny * tile_cols
        and tile_rows % ROWS == 0
        and tile_cols % 128 == 0
        and 2 * 5 * hidden * tile_rows * tile_cols * 2 <= 48 * 2**20
    )
    return channel_body(sizes, pair, *rest) if fits else gather_body(pair, *rest)


def solution(mesh):
    in_specs = (P(("grp", "gx", "gz"), "gy", None), P("grp"), P(), P(), P(), P(), P(), P(), P())
    out_specs = P(("grp", "gx", "gz"), "gy", None)
    sizes = (mesh.shape["gy"], mesh.shape["gx"], mesh.shape["gz"])
    return jax.shard_map(
        functools.partial(body, sizes), mesh=mesh, in_specs=in_specs, out_specs=out_specs, check_vma=False
    )
```

```python
import functools

import jax
import jax.numpy as jnp
from jax import lax
from jax.experimental import pallas as pl
from jax.experimental.pallas import tpu as pltpu
from jax.sharding import PartitionSpec as P

CHUNKS = 32
LAG = 2
DIRECT = 2
GROUPS = 4
ROWS = 32


def layer_norm(values, gain, bias):
    values = values.astype(jnp.float32)
    mean = jnp.mean(values, -1, keepdims=True)
    spread = jnp.mean(jnp.square(values - mean), -1, keepdims=True)
    return (values - mean) * lax.rsqrt(spread + 1e-05) * gain + bias


def channel_norm(values, gain, bias):
    mean = jnp.mean(values, 0, keepdims=True)
    spread = jnp.mean(jnp.square(values - mean), 0, keepdims=True)
    return (values - mean) * lax.rsqrt(spread + 1e-05) * gain[:, None, None] + bias[:, None, None]


def gather_body(pair, lengths, ln_gain, ln_bias, w_ab, w_gate, out_gain, out_bias, w_out):
    tile_rows, tile_cols, width = pair.shape
    hidden = w_out.shape[0]
    row_start = lax.axis_index(("gx", "gz")) * tile_rows
    col_index = lax.axis_index("gy")
    col_start = col_index * tile_cols
    normed = layer_norm(pair, ln_gain, ln_bias).astype(jnp.bfloat16)
    flat = normed.reshape(tile_rows * tile_cols, width)
    proj = jnp.dot(flat, w_ab, preferred_element_type=jnp.float32).reshape(
        tile_rows, tile_cols, 4 * hidden
    )
    row_live = (row_start + jnp.arange(tile_rows, dtype=jnp.int32) < lengths[0]).astype(jnp.float32)
    col_live = (col_start + jnp.arange(tile_cols, dtype=jnp.int32) < lengths[0]).astype(jnp.float32)
    pair_mask = (row_live[:, None] * col_live[None, :])[..., None]
    left = (pair_mask * jax.nn.sigmoid(proj[..., :hidden]) * proj[..., hidden : 2 * hidden]).astype(
        jnp.bfloat16
    )
    right = (
        pair_mask * jax.nn.sigmoid(proj[..., 2 * hidden : 3 * hidden]) * proj[..., 3 * hidden :]
    ).astype(jnp.bfloat16)
    left_major = jnp.transpose(left, (2, 0, 1))
    right_major = jnp.transpose(right, (2, 0, 1))
    column_rows = lax.all_gather(right_major, ("gx", "gz"), axis=1, tiled=True)
    right_mine = lax.all_to_all(column_rows, "gy", split_axis=1, concat_axis=2, tiled=True)
    triangle = jnp.einsum(
        "cik,cjk->cij",
        lax.all_gather(left_major, "gy", axis=2, tiled=True),
        right_mine,
        preferred_element_type=jnp.float32,
    )
    tri_norm = channel_norm(triangle, out_gain, out_bias).astype(jnp.bfloat16)
    gate = jax.nn.sigmoid(jnp.dot(flat, w_gate, preferred_element_type=jnp.float32)).reshape(
        tile_rows, tile_cols, width
    )
    projected = jnp.einsum("cij,cd->ijd", tri_norm, w_out, preferred_element_type=jnp.float32)
    return (gate * projected).astype(jnp.bfloat16)


def exchange_kernel(
    nx,
    nz,
    lengths,
    pair,
    gain,
    bias,
    w_ab,
    w_gate,
    out,
    gate_out,
    normed,
    send,
    gate_held,
    held,
    given,
    taken,
    deal_send,
    deal_recv,
    pass_send,
    pass_recv,
    cross_send,
    cross_recv,
    back_send,
    back_recv,
    own_sem,
    pair_sem,
    gate_sem,
    direct_send,
    direct_recv,
):
    nr = nx * nz
    hidden, rows, cols = send.shape[1:]
    width = pair.shape[2]
    blocks, lanes = rows // ROWS, ROWS * cols
    each = hidden // nr
    chunks = pass_send.shape[0]
    part = each // chunks
    gy, gx, gz = lax.axis_index("gy"), lax.axis_index("gx"), lax.axis_index("gz")
    me = gx * nz + gz
    half = gy // 2
    inner_plane, outer_plane = 1 + half, 3 * half
    inner = gy == inner_plane
    outer = jnp.logical_not(inner)

    def place(tall, plane):
        return {"gy": plane, "gx": tall // nz, "gz": tall % nz}

    def remote(src, dst, send_sem, recv_sem, device):
        return pltpu.make_async_remote_copy(
            src_ref=src,
            dst_ref=dst,
            send_sem=send_sem,
            recv_sem=recv_sem,
            device_id=device,
            device_id_type=pl.DeviceIdType.MESH,
        )

    def channels(chunk):
        return pl.ds(chunk * part, part)

    def band(tall):
        return pl.ds(pl.multiple_of(tall * rows, rows), rows)

    def columns(plane):
        return pl.ds(pl.multiple_of((plane - 2 * half) * cols, cols), cols)

    def deal(chunk, step):
        peer = lax.rem(me + step, nr)
        return remote(
            send.at[:, pl.ds(peer * each + chunk * part, part)],
            held.at[:, channels(chunk), band(me), pl.ds(0, cols)],
            deal_send.at[chunk, step],
            deal_recv.at[chunk, step],
            place(peer, gy),
        )

    def keep_in(chunk):
        return pltpu.make_async_copy(
            send.at[:, pl.ds(me * each + chunk * part, part)],
            held.at[:, channels(chunk), band(me), pl.ds(0, cols)],
            own_sem.at[0, chunk],
        )

    def pass_on(chunk):
        return remote(
            held.at[:, channels(chunk), :, pl.ds(0, cols)],
            held.at[:, channels(chunk), :, pl.ds(cols, cols)],
            pass_send.at[chunk],
            pass_recv.at[chunk],
            place(me, inner_plane),
        )

    def deal_inward(chunk, step):
        peer = lax.rem(me + step, nr)
        return remote(
            send.at[:, pl.ds(peer * each + chunk * part, part)],
            held.at[:, channels(chunk), band(me), pl.ds(cols, cols)],
            direct_send.at[chunk, step],
            direct_recv.at[chunk, step],
            place(peer, inner_plane),
        )

    def cross(chunk):
        return remote(
            given.at[channels(chunk)],
            taken.at[channels(chunk)],
            cross_send.at[chunk],
            cross_recv.at[chunk],
            place(me, 3 - gy),
        )

    def hand_back(chunk, step, plane, side):
        peer = lax.rem(me + step, nr)
        return remote(
            taken.at[channels(chunk), band(peer), columns(plane)],
            out.at[pl.ds(me * each + chunk * part, part)],
            back_send.at[side, chunk, step],
            back_recv.at[chunk, step],
            place(peer, plane),
        )

    def keep_out(chunk):
        return pltpu.make_async_copy(
            taken.at[channels(chunk), band(me), columns(inner_plane)],
            out.at[pl.ds(me * each + chunk * part, part)],
            own_sem.at[1, chunk],
        )

    def load(block):
        return pltpu.make_async_copy(
            pair.at[pl.ds(block * ROWS, ROWS)],
            normed.at[pl.ds(block * ROWS, ROWS)],
            pair_sem.at[block],
        )

    for block in range(blocks):
        load(block).start()
    barrier = pltpu.get_barrier_semaphore()
    total = 4 * nr
    index = gy * nr + me
    for step in range(1, total):
        peer = lax.rem(index + step, total)
        pl.semaphore_signal(
            barrier,
            inc=1,
            device_id=place(peer % nr, peer // nr),
            device_id_type=pl.DeviceIdType.MESH,
        )
    def dealt(chunk):
        for step in range(1, nr):
            deal(chunk, step).wait_recv()
        keep_in(chunk).wait()

    def product(channel, which):
        below = pl.ds(pl.multiple_of(which * 2 * cols, 2 * cols), 2 * cols)
        return lax.dot_general(
            held[0, channel],
            held[1, channel, below, :],
            (((1,), (1,)), ((), ())),
            preferred_element_type=jnp.float32,
        )

    @pl.loop(0, blocks)
    def _(block):
        load(block).wait()
        here = pl.ds(pl.multiple_of(block * ROWS, ROWS), ROWS)
        flat = normed[here].reshape(lanes, width)
        value = layer_norm(flat, gain[...], bias[...]).astype(jnp.bfloat16)
        normed[here] = value.reshape(ROWS, cols, width)

    upright_w = jnp.transpose(w_ab[...].astype(jnp.float32))
    lane = lax.broadcasted_iota(jnp.int32, (1, lanes), 1)
    col_live = gy * cols + lane % cols < lengths[0]
    span = each // GROUPS

    def project(group):
        starts = [
            kind * hidden + tall * each + group * span for kind in range(4) for tall in range(nr)
        ]
        weights = jnp.concatenate([upright_w[at : at + span] for at in starts]).astype(jnp.bfloat16)
        height = nr * span

        @pl.loop(0, blocks)
        def _(block):
            here = pl.ds(pl.multiple_of(block * ROWS, ROWS), ROWS)
            proj = lax.dot_general(
                weights,
                normed[here].reshape(lanes, width),
                (((1,), (1,)), ((), ())),
                preferred_element_type=jnp.float32,
            )
            row_live = me * rows + block * ROWS + lane // cols < lengths[0]
            mask = (row_live & col_live).astype(jnp.float32)
            for side in range(2):
                gates = proj[2 * side * height : (2 * side + 1) * height]
                values = proj[(2 * side + 1) * height : (2 * side + 2) * height]
                value = mask * jax.nn.sigmoid(gates) * values
                value = value.reshape(height, ROWS, cols).astype(jnp.bfloat16)
                for tall in range(nr):
                    first = tall * each + group * span
                    send[side, first : first + span, here] = value[tall * span : (tall + 1) * span]

        if group == 0:
            pl.semaphore_wait(barrier, total - 1)

        @pl.loop(group * span // part, (group + 1) * span // part)
        def _(chunk):
            direct = outer & (chunk < DIRECT)

            @pl.when(direct)
            def _():
                for step in range(nr):
                    deal_inward(chunk, step).start()

            @pl.when(jnp.logical_not(direct))
            def _():
                for step in range(1, nr):
                    deal(chunk, step).start()
                keep_in(chunk).start()

    for group in range(GROUPS):
        project(group)
        if group:

            @pl.when(outer)
            def _():
                dealt(DIRECT + group - 1)
                pass_on(DIRECT + group - 1).start()

    def store_gate(block):
        return pltpu.make_async_copy(
            gate_held.at[block % 2],
            gate_out.at[pl.ds(block * ROWS, ROWS)],
            gate_sem.at[block % 2],
        )

    def gate_turn(turn):
        block = turn - 2 * GROUPS

        @pl.when((block >= 2) & (block < blocks + 2))
        def _():
            store_gate(block - 2).wait()

        @pl.when((block >= 0) & (block < blocks))
        def _():
            here = pl.ds(pl.multiple_of(block * ROWS, ROWS), ROWS)
            value = jax.nn.sigmoid(
                jnp.dot(
                    normed[here].reshape(lanes, width),
                    w_gate[...],
                    preferred_element_type=jnp.float32,
                )
            )
            gate_held[block % 2] = value.reshape(ROWS, cols, width)
            store_gate(block).start()

    @pl.when(outer)
    def _():
        @pl.loop(DIRECT + GROUPS - 1, chunks)
        def _(chunk):
            dealt(chunk)
            pass_on(chunk).start()
            gate_turn(chunk)

        @pl.loop(0, chunks)
        def _(chunk):
            for step in range(nr):
                hand_back(chunk, step, outer_plane, 1).wait_recv()

            @pl.when(chunk < DIRECT)
            def _():
                for step in range(nr):
                    deal_inward(chunk, step).wait_send()

            @pl.when(chunk >= DIRECT)
            def _():
                for step in range(1, nr):
                    deal(chunk, step).wait_send()
                pass_on(chunk).wait_send()

    @pl.when(inner)
    def _():
        @pl.loop(0, chunks + LAG)
        def _(turn):
            @pl.when(turn < chunks)
            def _():
                dealt(turn)

                @pl.when(turn < DIRECT)
                def _():
                    for step in range(nr):
                        deal_inward(turn, step).wait_recv()

                @pl.when(turn >= DIRECT)
                def _():
                    pass_on(turn).wait_recv()


                @pl.loop(turn * part, (turn + 1) * part)
                def _(channel):
                    given[channel] = product(channel, 1 - half).astype(jnp.bfloat16)

                cross(turn).start()

            @pl.when(turn >= LAG)
            def _():
                chunk = turn - LAG
                cross(chunk).wait_recv()

                @pl.loop(chunk * part, (chunk + 1) * part)
                def _(channel):
                    total = product(channel, half) + taken[channel].astype(jnp.float32)
                    taken[channel] = total.astype(jnp.bfloat16)

                for step in range(nr):
                    hand_back(chunk, step, outer_plane, 1).start()
                for step in range(1, nr):
                    hand_back(chunk, step, inner_plane, 0).start()
                keep_out(chunk).start()

            gate_turn(turn)

        @pl.loop(0, chunks)
        def _(chunk):
            for step in range(1, nr):
                hand_back(chunk, step, inner_plane, 0).wait_recv()
                hand_back(chunk, step, inner_plane, 0).wait_send()
                deal(chunk, step).wait_send()
            for step in range(nr):
                hand_back(chunk, step, outer_plane, 1).wait_send()
            cross(chunk).wait_send()
            keep_out(chunk).wait()


def upright(row):
    return jnp.transpose(jnp.broadcast_to(row[...], (row.shape[1], row.shape[1])))[:, :1]


def finish_kernel(gate, tri, out_gain, out_bias, w_out, out):
    rows, cols, width = out.shape
    hidden = tri.shape[0]
    values = tri[...].astype(jnp.float32)
    mean = jnp.mean(values, 0, keepdims=True)
    centred = values - mean
    spread = jnp.mean(jnp.square(centred), 0, keepdims=True)
    scaled = (centred * lax.rsqrt(spread + 1e-05)).reshape(hidden, rows * cols)
    tri_norm = (scaled * upright(out_gain) + upright(out_bias)).astype(jnp.bfloat16)
    projected = lax.dot_general(
        tri_norm, w_out[...], (((0,), (0,)), ((), ())), preferred_element_type=jnp.float32
    )
    out[...] = (gate[...] * projected.reshape(rows, cols, width)).astype(jnp.bfloat16)


def whole(shape):
    return pl.BlockSpec(shape, lambda step: (0,) * len(shape))


def channel_body(sizes, pair, lengths, ln_gain, ln_bias, w_ab, w_gate, out_gain, out_bias, w_out):
    ny, nx, nz = sizes
    tile_rows, tile_cols, width = pair.shape
    hidden = w_out.shape[0]
    gain, bias = ln_gain[None, :], ln_bias[None, :]
    smem = pl.BlockSpec(memory_space=pltpu.SMEM)
    steps = tile_rows // ROWS
    dma = pltpu.SemaphoreType.DMA
    any_space = pl.BlockSpec(memory_space=pl.ANY)
    nr = nx * nz
    each, side = hidden // nr, nr * tile_rows
    vmem = pl.BlockSpec(memory_space=pltpu.VMEM)
    triangle, gate = pl.pallas_call(
        functools.partial(exchange_kernel, nx, nz),
        name="exchange",
        out_shape=(
            jax.ShapeDtypeStruct((hidden, tile_rows, tile_cols), jnp.bfloat16),
            jax.ShapeDtypeStruct(pair.shape, jnp.float32),
        ),
        in_specs=[smem, any_space, vmem, vmem, vmem, vmem],
        out_specs=(any_space, any_space),
        scratch_shapes=[
            pltpu.VMEM(pair.shape, jnp.bfloat16),
            pltpu.VMEM((2, hidden, tile_rows, tile_cols), jnp.bfloat16),
            pltpu.VMEM((2, ROWS, tile_cols, width), jnp.float32),
            pltpu.VMEM((2, each, side, 2 * tile_cols), jnp.bfloat16),
            pltpu.VMEM((each, side, 2 * tile_cols), jnp.bfloat16),
            pltpu.VMEM((each, side, 2 * tile_cols), jnp.bfloat16),
            dma((CHUNKS, nr)),
            dma((CHUNKS, nr)),
            dma((CHUNKS,)),
            dma((CHUNKS,)),
            dma((CHUNKS,)),
            dma((CHUNKS,)),
            dma((2, CHUNKS, nr)),
            dma((CHUNKS, nr)),
            dma((2, CHUNKS)),
            dma((steps,)),
            dma((2,)),
            dma((DIRECT, nr)),
            dma((DIRECT, nr)),
        ],
        compiler_params=pltpu.CompilerParams(
            collective_id=0, has_side_effects=True, vmem_limit_bytes=63 * 2**20
        ),
    )(lengths, pair, gain, bias, w_ab, w_gate)
    return pl.pallas_call(
        finish_kernel,
        name="finish",
        grid=(steps,),
        out_shape=jax.ShapeDtypeStruct(pair.shape, jnp.bfloat16),
        in_specs=[
            pl.BlockSpec((ROWS, tile_cols, width), lambda step: (step, 0, 0)),
            pl.BlockSpec((hidden, ROWS, tile_cols), lambda step: (0, step, 0)),
            whole((1, hidden)),
            whole((1, hidden)),
            whole((hidden, width)),
        ],
        out_specs=pl.BlockSpec((ROWS, tile_cols, width), lambda step: (step, 0, 0)),
        compiler_params=pltpu.CompilerParams(vmem_limit_bytes=56 * 2**20),
    )(gate, triangle, out_gain[None, :], out_bias[None, :], w_out)


def body(sizes, pair, *rest):
    ny, nx, nz = sizes
    hidden = rest[-1].shape[0]
    tile_rows, tile_cols, _ = pair.shape
    fits = (
        ny == 4
        and hidden % (nx * nz * CHUNKS) == 0
        and hidden % (nx * nz * GROUPS * 8) == 0
        and nx * nz * tile_rows == ny * tile_cols
        and tile_rows % ROWS == 0
        and tile_cols % 128 == 0
        and 2 * 5 * hidden * tile_rows * tile_cols * 2 <= 48 * 2**20
    )
    return channel_body(sizes, pair, *rest) if fits else gather_body(pair, *rest)


def solution(mesh):
    in_specs = (P(("grp", "gx", "gz"), "gy", None), P("grp"), P(), P(), P(), P(), P(), P(), P())
    out_specs = P(("grp", "gx", "gz"), "gy", None)
    sizes = (mesh.shape["gy"], mesh.shape["gx"], mesh.shape["gz"])
    return jax.shard_map(
        functools.partial(body, sizes), mesh=mesh, in_specs=in_specs, out_specs=out_specs, check_vma=False
    )
```
